8 devices in a mesh: dp: 2 (over z, y), tp: 4 (over x, core).
Axes of the slice: x: 2, y: 2, z: 1, core: 2. Of those that a mesh axis runs over, the one named last changes fastest.
Arguments:
- x: bfloat16 [640, 3072], P('dp'), parts along dimension 0
- lengths: int32 [130], P('dp'), parts along dimension 0
- attn_gain: bfloat16 [2, 3072], replicated
- w_q: bfloat16 [2, 3072, 3072], P(None, None, 'tp')
- w_k: bfloat16 [2, 3072, 1024], P(None, None, 'tp')
- w_v: bfloat16 [2, 3072, 1024], P(None, None, 'tp')
- w_o: bfloat16 [2, 3072, 3072], P(None, 'tp')
- mlp_gain: bfloat16 [2, 3072], replicated
- w_gate: bfloat16 [2, 3072, 8192], P(None, None, 'tp')
- w_up: bfloat16 [2, 3072, 8192], P(None, None, 'tp')
- w_down: bfloat16 [2, 8192, 3072], P(None, 'tp')
- k_cache: bfloat16 [2, 130, 8, 1024, 128], P(None, 'dp', 'tp'), parts along dimension 1
- v_cache: bfloat16 [2, 130, 8, 1024, 128], P(None, 'dp', 'tp'), parts along dimension 1
Outputs:
- output: bfloat16 [640, 3072], P('dp'), parts along dimension 0
There are 2 independent parts. The reference program is written for one: setup_inputs(seed, part) draws one part's arguments, and reference() takes and returns one part's arrays. A program takes and returns all parts, laid end to end along the dimension named above; an argument that names none is the same for every part.
All inputs are finite; a program needn't handle non-finite values.
Results may differ from the reference program's by a relative error of at most 0.0197503.
Values are sent between devices in bfloat16 or wider.
A program may use at most 1 GiB of HBM per device.

```python
import jax
import jax.numpy as jnp
from jax import lax

D = 3072
HEADS = 24
KV_HEADS = 8
HEAD = 128
FF = 8192
BATCH = 64
CHUNK = 256
SEQ = 1024
LAYERS = 2

GROUP = HEADS // KV_HEADS
TOKENS = BATCH + CHUNK
ATTN_SCALE = HEAD ** -0.5
ROPE_BASE = 500000.0
EPSILON = 1e-5


def setup_inputs(seed: int = 0, part: int = 0) -> dict:
    root_key = jax.random.key(seed)
    shared_keys = jax.random.split(root_key, 9)
    part_keys = jax.random.split(jax.random.fold_in(root_key, part), 8)

    def gaussian(sub_key, arr_shape, factor):
        return jax.random.normal(sub_key, arr_shape, jnp.float32) * factor

    lengths = jax.random.randint(part_keys[1], (BATCH + 1,), 1, SEQ)
    longest = jax.random.randint(part_keys[2], (), 0, BATCH + 1)
    lengths = jnp.where(jnp.arange(BATCH + 1) == longest, SEQ - 1, lengths).astype(jnp.int32)
    pos_ramp = (jnp.arange(SEQ, dtype=jnp.float32) * (2.0 / SEQ) - 1.0)[:, None]
    cache_shape = (LAYERS, BATCH + 1, KV_HEADS, SEQ, HEAD)
    row_shape = (LAYERS, BATCH + 1, KV_HEADS, 1, HEAD)
    k_cache = gaussian(part_keys[3], cache_shape, 1.0) + pos_ramp * gaussian(part_keys[4], row_shape, 1.0)
    v_cache = gaussian(part_keys[5], row_shape, 1.0) + pos_ramp * gaussian(part_keys[6], row_shape, 1.0) + gaussian(part_keys[7], cache_shape, 0.5)
    return {
        'x': gaussian(part_keys[0], (TOKENS, D), 1.0).astype(jnp.bfloat16),
        'lengths': lengths,
        'attn_gain': jax.random.uniform(shared_keys[0], (LAYERS, D), jnp.float32, 0.5, 1.5).astype(jnp.bfloat16),
        'w_q': gaussian(shared_keys[1], (LAYERS, D, HEADS * HEAD), D ** -0.5).astype(jnp.bfloat16),
        'w_k': gaussian(shared_keys[2], (LAYERS, D, KV_HEADS * HEAD), D ** -0.5).astype(jnp.bfloat16),
        'w_v': gaussian(shared_keys[3], (LAYERS, D, KV_HEADS * HEAD), D ** -0.5).astype(jnp.bfloat16),
        'w_o': gaussian(shared_keys[4], (LAYERS, HEADS * HEAD, D), (HEADS * HEAD) ** -0.5).astype(jnp.bfloat16),
        'mlp_gain': jax.random.uniform(shared_keys[5], (LAYERS, D), jnp.float32, 0.5, 1.5).astype(jnp.bfloat16),
        'w_gate': gaussian(shared_keys[6], (LAYERS, D, FF), D ** -0.5).astype(jnp.bfloat16),
        'w_up': gaussian(shared_keys[7], (LAYERS, D, FF), D ** -0.5).astype(jnp.bfloat16),
        'w_down': gaussian(shared_keys[8], (LAYERS, FF, D), 1.5 * FF ** -0.5).astype(jnp.bfloat16),
        'k_cache': k_cache.astype(jnp.bfloat16),
        'v_cache': v_cache.astype(jnp.bfloat16),
    }


def rms_norm(x, norm_gain):
    x_f32 = x.astype(jnp.float32)
    inv_rms = lax.rsqrt(jnp.mean(x_f32 * x_f32, axis=-1, keepdims=True) + EPSILON)
    return (x_f32 * inv_rms * norm_gain.astype(jnp.float32)).astype(jnp.bfloat16)


def rope_tables(positions):
    freq_exps = jnp.arange(0, HEAD, 2, dtype=jnp.float32) / HEAD
    angles = positions.astype(jnp.float32)[:, None] * jnp.power(ROPE_BASE, -freq_exps)[None, :]
    return jnp.cos(angles)[:, None, :], jnp.sin(angles)[:, None, :]


def apply_rope(vectors, cos_tab, sin_tab):
    half_dim = HEAD // 2
    vec_f32 = vectors.astype(jnp.float32)
    first = vec_f32[..., :half_dim]
    second = vec_f32[..., half_dim:]
    return jnp.concatenate([first * cos_tab - second * sin_tab, second * cos_tab + first * sin_tab], axis=-1).astype(jnp.bfloat16)


def decode_row(row_args):
    q_row, k_row, v_row, kc_row, vc_row, length = row_args
    q_f32 = q_row.reshape(KV_HEADS, GROUP, HEAD).astype(jnp.float32)
    logits_cache = jnp.einsum('grd,gsd->grs', q_f32, kc_row.astype(jnp.float32)) * ATTN_SCALE
    logits_cache = jnp.where(jnp.arange(SEQ)[None, None, :] < length, logits_cache, -jnp.inf)
    logits_self = jnp.einsum('grd,gd->gr', q_f32, k_row.astype(jnp.float32))[:, :, None] * ATTN_SCALE
    prob_all = jax.nn.softmax(jnp.concatenate([logits_cache, logits_self], axis=-1), axis=-1)
    prob_all = prob_all.astype(jnp.bfloat16).astype(jnp.float32)
    result = jnp.einsum('grs,gsd->grd', prob_all[..., :SEQ], vc_row.astype(jnp.float32)) + prob_all[..., SEQ:] * v_row.astype(jnp.float32)[:, None, :]
    return result.astype(jnp.bfloat16).reshape(HEADS * HEAD)


def chunk_attention(q_chk, k_chk, v_chk, kc_row, vc_row, prefix_len):
    q_heads = q_chk.reshape(CHUNK, KV_HEADS, GROUP, HEAD).transpose(1, 0, 2, 3)
    k_heads = k_chk.transpose(1, 0, 2)
    v_heads = v_chk.transpose(1, 0, 2)
    cache_mask = jnp.arange(SEQ)[None, None, :] < prefix_len
    tok_ids = jnp.arange(CHUNK)
    causal_mask = (tok_ids[None, :] <= tok_ids[:, None])[:, None, :]

    def one_head(head_args):
        q_head, k_head, v_head, kc_head, vc_head = head_args
        q_f32 = q_head.astype(jnp.float32)
        logits_cache = jnp.einsum('crd,sd->crs', q_f32, kc_head.astype(jnp.float32)) * ATTN_SCALE
        logits_cache = jnp.where(cache_mask, logits_cache, -jnp.inf)
        logits_new = jnp.einsum('crd,jd->crj', q_f32, k_head.astype(jnp.float32)) * ATTN_SCALE
        logits_new = jnp.where(causal_mask, logits_new, -jnp.inf)
        prob_all = jax.nn.softmax(jnp.concatenate([logits_cache, logits_new], axis=-1), axis=-1)
        prob_all = prob_all.astype(jnp.bfloat16).astype(jnp.float32)
        result = jnp.einsum('crs,sd->crd', prob_all[..., :SEQ], vc_head.astype(jnp.float32)) + jnp.einsum('crj,jd->crd', prob_all[..., SEQ:], v_head.astype(jnp.float32))
        return result.astype(jnp.bfloat16)

    heads_out = lax.map(one_head, (q_heads, k_heads, v_heads, kc_row, vc_row))
    return heads_out.transpose(1, 0, 2, 3).reshape(CHUNK, HEADS * HEAD)


def decoder_layer(x, lengths, cos_tab, sin_tab, params):
    attn_gain, w_q, w_k, w_v, w_o, mlp_gain, w_gate, w_up, w_down, k_cache, v_cache = params
    normed = rms_norm(x, attn_gain)
    q_all = apply_rope(jnp.dot(normed, w_q, preferred_element_type=jnp.float32).astype(jnp.bfloat16).reshape(TOKENS, HEADS, HEAD), cos_tab, sin_tab)
    k_all = apply_rope(jnp.dot(normed, w_k, preferred_element_type=jnp.float32).astype(jnp.bfloat16).reshape(TOKENS, KV_HEADS, HEAD), cos_tab, sin_tab)
    v_all = jnp.dot(normed, w_v, preferred_element_type=jnp.float32).astype(jnp.bfloat16).reshape(TOKENS, KV_HEADS, HEAD)
    dec_out = lax.map(decode_row, (q_all[:BATCH], k_all[:BATCH], v_all[:BATCH], k_cache[:BATCH], v_cache[:BATCH], lengths[:BATCH]))
    chk_out = chunk_attention(q_all[BATCH:], k_all[BATCH:], v_all[BATCH:], k_cache[BATCH], v_cache[BATCH], lengths[BATCH])
    attended = jnp.concatenate([dec_out, chk_out], axis=0)
    hidden = (x.astype(jnp.float32) + jnp.dot(attended, w_o, preferred_element_type=jnp.float32)).astype(jnp.bfloat16)
    mlp_in = rms_norm(hidden, mlp_gain)
    gate_proj = jnp.dot(mlp_in, w_gate, preferred_element_type=jnp.float32)
    up_proj = jnp.dot(mlp_in, w_up, preferred_element_type=jnp.float32)
    activated = (jax.nn.silu(gate_proj) * up_proj).astype(jnp.bfloat16)
    down_proj = jnp.dot(activated, w_down, preferred_element_type=jnp.float32)
    return (hidden.astype(jnp.float32) + down_proj).astype(jnp.bfloat16)


def reference(x, lengths, attn_gain, w_q, w_k, w_v, w_o, mlp_gain, w_gate, w_up, w_down, k_cache, v_cache):
    positions = jnp.concatenate([lengths[:BATCH], lengths[BATCH] + jnp.arange(CHUNK, dtype=jnp.int32)])
    cos_tab, sin_tab = rope_tables(positions)

    def layer_step(hidden, params):
        return decoder_layer(hidden, lengths, cos_tab, sin_tab, params), None

    result, unused = lax.scan(layer_step, x, (attn_gain, w_q, w_k, w_v, w_o, mlp_gain, w_gate, w_up, w_down, k_cache, v_cache))
    return result
```

```python
import functools

import jax
import jax.numpy as jnp
from jax import lax
from jax.experimental import pallas as pl
from jax.experimental.pallas import tpu as pltpu
from jax.sharding import PartitionSpec as P

ROPE_BASE = 500000.0
EPSILON = 1e-5
MESH = pl.DeviceIdType.MESH
F32 = jnp.float32
BF16 = jnp.bfloat16
VMEM_LIMIT = 66_900_000
TILE = 256
GROUPS = ((0, 160), (160, 160))


def rope_tables(positions, head_dim):
    freq_exps = jnp.arange(0, head_dim, 2, dtype=F32) / head_dim
    angles = positions.astype(F32)[:, None] * jnp.power(ROPE_BASE, -freq_exps)[None, :]
    cos_half, sin_half = jnp.cos(angles), jnp.sin(angles)
    return jnp.concatenate([cos_half, cos_half], axis=-1), jnp.concatenate([-sin_half, sin_half], axis=-1)


def norm_rows(h_ref, gain, b_ref, row0, rows, block=16):
    half = h_ref.shape[2]
    gain_lo, gain_hi = gain[:, :half], gain[:, half:]

    def step(i, _):
        src = pl.ds(pl.multiple_of(row0 + i * block, block), block)
        dst = pl.ds(pl.multiple_of(i * block, block), block)
        lo, hi = h_ref[0, src, :].astype(F32), h_ref[1, src, :].astype(F32)
        total = jnp.sum(lo * lo, axis=-1, keepdims=True) + jnp.sum(hi * hi, axis=-1, keepdims=True)
        inv = lax.rsqrt(total / (2 * half) + EPSILON)
        b_ref[dst, :half] = (lo * inv * gain_lo).astype(BF16)
        b_ref[dst, half:] = (hi * inv * gain_hi).astype(BF16)
        return 0

    lax.fori_loop(0, rows // block, step, 0)


def rope_store(prod, cos, sin, out_ref, rows, col):
    head = cos.shape[1]
    for k in range(prod.shape[1] // head):
        vec = prod[:, k * head:(k + 1) * head].astype(BF16).astype(F32)
        rot = vec * cos + pltpu.roll(vec, head // 2, 1) * sin
        out_ref[rows, pl.ds(col + k * head, head)] = rot.astype(BF16)


def qkv_rows(b_ref, wq_ref, wk_ref, wv_ref, cos_ref, sin_ref, q_ref, k_ref, v_ref, row0, rows):
    rows_at = pl.ds(row0, rows)
    lhs = b_ref[0:rows, :]
    cos, sin = cos_ref[rows_at, :], sin_ref[rows_at, :]

    def q_tile(j, _):
        col = pl.multiple_of(j * TILE, TILE)
        prod = jnp.dot(b_ref[0:rows, :], wq_ref[:, pl.ds(col, TILE)], preferred_element_type=F32)
        rope_store(prod, cos_ref[rows_at, :], sin_ref[rows_at, :], q_ref, rows_at, col)
        return 0

    lax.fori_loop(0, wq_ref.shape[1] // TILE, q_tile, 0)
    rope_store(jnp.dot(lhs, wk_ref[...], preferred_element_type=F32), cos, sin, k_ref, rows_at, 0)
    v_ref[rows_at, :] = jnp.dot(lhs, wv_ref[...], preferred_element_type=F32).astype(BF16)


def qkv_kernel(x_hbm, gain_ref, cos_ref, sin_ref, wq_hbm, wk_hbm, wv_hbm, q_ref, k_ref, v_ref, h, b, wq, wk, wv, sems):
    half = h.shape[2]
    copies = [pltpu.make_async_copy(x_hbm.at[:, pl.ds(s * half, half)], h.at[s], sems.at[s]) for s in range(2)]
    copies += [pltpu.make_async_copy(src.at[0], dst, sems.at[2 + n]) for n, (src, dst) in enumerate(((wq_hbm, wq), (wk_hbm, wk), (wv_hbm, wv)))]
    for copy in copies:
        copy.start()
    copies[0].wait()
    copies[1].wait()
    rows = h.shape[1]
    norm_rows(h, gain_ref[...].astype(F32)[0:1, :], b, 0, rows)
    for copy in copies[2:]:
        copy.wait()
    qkv_rows(b, wq, wk, wv, cos_ref, sin_ref, q_ref, k_ref, v_ref, 0, rows)


def qkv_call(x, gain, cos, sin, w_q, w_k, w_v):
    rows, width = x.shape
    vmem = pl.BlockSpec(memory_space=pltpu.VMEM)
    hbm = pl.BlockSpec(memory_space=pl.ANY)
    return pl.pallas_call(
        qkv_kernel,
        name='qkv_first',
        out_shape=[jax.ShapeDtypeStruct((rows, w.shape[2]), BF16) for w in (w_q, w_k, w_v)],
        in_specs=[hbm, vmem, vmem, vmem, hbm, hbm, hbm],
        out_specs=[vmem] * 3,
        scratch_shapes=[
            pltpu.VMEM((2, rows, width // 2), BF16),
            pltpu.VMEM((rows, width), BF16),
            pltpu.VMEM(w_q.shape[1:], BF16),
            pltpu.VMEM(w_k.shape[1:], BF16),
            pltpu.VMEM(w_v.shape[1:], BF16),
            pltpu.SemaphoreType.DMA((5,)),
        ],
        compiler_params=pltpu.CompilerParams(vmem_limit_bytes=40 * 2**20),
    )(x, gain, cos, sin, w_q, w_k, w_v)


UNIT = 128
BATCH = 8
BITS = (8, 4, 2, 1)


def attention_kernel(layer, len_ref, q_ref, k_ref, v_ref, kc_hbm, vc_hbm, o_ref, kbuf, vbuf, qs, kf, vf, sc, od, kp, vp, sems, psems):
    rows = kc_hbm.shape[1] - 1
    seq, head = kc_hbm.shape[3], kc_hbm.shape[4]
    heads = q_ref.shape[1] // head
    kv = kc_hbm.shape[2]
    rep = heads // kv
    chunk = q_ref.shape[0] - rows
    scale = head ** -0.5
    steps = rows // BATCH

    def copies(step, slot, act):
        for i in range(BATCH):
            row = step * BATCH + i
            units = (len_ref[row] + UNIT - 1) // UNIT
            for n, bit in enumerate(BITS):
                @pl.when((units // bit) % 2 == 1)
                def _(i=i, row=row, units=units, n=n, bit=bit):
                    off = pl.multiple_of((units // (2 * bit)) * (2 * bit * UNIT), UNIT)
                    span = pl.ds(off, bit * UNIT)
                    for m, (src, dst) in enumerate(((kc_hbm, kbuf), (vc_hbm, vbuf))):
                        copy = pltpu.make_async_copy(src.at[layer, row, :, span, :], dst.at[slot, i, :, span, :], sems.at[slot, i, n, m])
                        if act == 'start':
                            copy.start()
                        else:
                            copy.wait()

    prefill = [pltpu.make_async_copy(src.at[layer, rows], dst, psems.at[n]) for n, (src, dst) in enumerate(((kc_hbm, kp), (vc_hbm, vp)))]
    for copy in prefill:
        copy.start()

    def clear(i, _):
        for slot in range(2):
            for g in range(kv):
                vbuf[slot, i, g] = jnp.zeros((seq, head), BF16)
        return 0

    lax.fori_loop(0, BATCH, clear, 0)
    copies(0, 0, 'start')

    qs[...] = jnp.zeros_like(qs)
    for h in range(heads):
        qs[h // rep, pl.ds(h, rows, stride=8), :] = q_ref[0:rows, h * head:(h + 1) * head].astype(F32)
    kf[...] = k_ref[0:rows, :].astype(F32)
    vf[...] = v_ref[0:rows, :].astype(F32)

    for copy in prefill:
        copy.wait()
    limit = len_ref[rows]

    def prefill_head(h, _):
        g = h // rep
        q = q_ref[rows:, pl.ds(pl.multiple_of(h * head, head), head)]
        kn = k_ref[rows:, pl.ds(pl.multiple_of(g * head, head), head)]
        vn = v_ref[rows:, pl.ds(pl.multiple_of(g * head, head), head)]
        dims = (((1,), (1,)), ((), ()))
        s_old = lax.dot_general(q, kp[g], dims, preferred_element_type=F32) * scale
        s_new = lax.dot_general(q, kn, dims, preferred_element_type=F32) * scale
        s_old = jnp.where(lax.broadcasted_iota(jnp.int32, s_old.shape, 1) < limit, s_old, -jnp.inf)
        causal = lax.broadcasted_iota(jnp.int32, s_new.shape, 1) <= lax.broadcasted_iota(jnp.int32, s_new.shape, 0)
        s_new = jnp.where(causal, s_new, -jnp.inf)
        top = jnp.maximum(jnp.max(s_old, axis=-1, keepdims=True), jnp.max(s_new, axis=-1, keepdims=True))
        e_old, e_new = jnp.exp(s_old - top), jnp.exp(s_new - top)
        inv = 1.0 / (jnp.sum(e_old, axis=-1, keepdims=True) + jnp.sum(e_new, axis=-1, keepdims=True))
        out = jnp.dot((e_old * inv).astype(BF16), vp[g], preferred_element_type=F32)
        out += jnp.dot((e_new * inv).astype(BF16), vn, preferred_element_type=F32)
        o_ref[rows:, pl.ds(pl.multiple_of(h * head, head), head)] = out.astype(BF16)
        return 0

    lax.fori_loop(0, heads, prefill_head, 0)

    def decode_step(step, _):
        slot = lax.rem(step, 2)

        @pl.when(step + 1 < steps)
        def _():
            copies(step + 1, 1 - slot, 'start')

        copies(step, slot, 'wait')
        for i in range(BATCH):
            row = step * BATCH + i
            length = len_ref[row]
            base = pl.multiple_of((length // 16) * 16, 16)
            hit = lax.broadcasted_iota(jnp.int32, (16, head), 0) == length - base
            for buf, new in ((kbuf, kf), (vbuf, vf)):
                for g in range(kv):
                    old = buf[slot, i, g, pl.ds(base, 16), :].astype(F32)
                    mine = new[pl.ds(pl.multiple_of(step * BATCH, BATCH), BATCH), g * head:(g + 1) * head][i:i + 1, :]
                    buf[slot, i, g, pl.ds(base, 16), :] = jnp.where(hit, mine, old).astype(BF16)
        for i in range(BATCH):
            row = step * BATCH + i
            at = pl.ds(pl.multiple_of(row * 8, 8), 8)
            q = jnp.concatenate([qs[g, at, :] for g in range(kv)], axis=-1).astype(BF16)
            keys = jnp.concatenate([kbuf[slot, i, g] for g in range(kv)], axis=-1)
            s = lax.dot_general(q, keys, (((1,), (1,)), ((), ())), preferred_element_type=F32) * scale
            s = jnp.where(lax.broadcasted_iota(jnp.int32, s.shape, 1) <= len_ref[row], s, -jnp.inf)
            sc[i * 8:(i + 1) * 8, :] = s
        for i in range(BATCH):
            s = sc[i * 8:(i + 1) * 8, :]
            e = jnp.exp(s - jnp.max(s, axis=-1, keepdims=True))
            p = (e * (1.0 / jnp.sum(e, axis=-1, keepdims=True))).astype(BF16)
            values = jnp.concatenate([vbuf[slot, i, g] for g in range(kv)], axis=-1)
            o = jnp.dot(p, values, preferred_element_type=F32)
            own = lax.broadcasted_iota(jnp.int32, (8, head), 0) // rep
            pick = o[:, 0:head]
            for g in range(1, kv):
                pick = jnp.where(own == g, o[:, g * head:(g + 1) * head], pick)
            row = step * BATCH + i
            od[pl.ds(pl.multiple_of(row * 8, 8), 8), :] = pick
        return 0

    lax.fori_loop(0, steps, decode_step, 0)
    for h in range(heads):
        o_ref[0:rows, h * head:(h + 1) * head] = od[pl.ds(h, rows, stride=8), :].astype(BF16)


def attention_call(layer, lengths, q, k, v, k_cache, v_cache):
    rows = k_cache.shape[1] - 1
    kv, seq, head = k_cache.shape[2:]
    vmem = pl.BlockSpec(memory_space=pltpu.VMEM)
    hbm = pl.BlockSpec(memory_space=pl.ANY)
    return pl.pallas_call(
        functools.partial(attention_kernel, layer),
        name=f'attention_{layer}',
        out_shape=jax.ShapeDtypeStruct(q.shape, BF16),
        in_specs=[pl.BlockSpec(memory_space=pltpu.SMEM), vmem, vmem, vmem, hbm, hbm],
        out_specs=vmem,
        scratch_shapes=[
            pltpu.VMEM((2, BATCH, kv, seq, head), BF16),
            pltpu.VMEM((2, BATCH, kv, seq, head), BF16),
            pltpu.VMEM((kv, rows * 8, head), F32),
            pltpu.VMEM((rows, kv * head), F32),
            pltpu.VMEM((rows, kv * head), F32),
            pltpu.VMEM((BATCH * 8, seq), F32),
            pltpu.VMEM((rows * 8, head), F32),
            pltpu.VMEM((kv, seq, head), BF16),
            pltpu.VMEM((kv, seq, head), BF16),
            pltpu.SemaphoreType.DMA((2, BATCH, len(BITS), 2)),
            pltpu.SemaphoreType.DMA((2,)),
        ],
        compiler_params=pltpu.CompilerParams(vmem_limit_bytes=48 * 2**20),
    )(lengths, q, k, v, k_cache, v_cache)


def block_kernel(layer, last, groups, *refs):
    if last:
        (x_hbm, att_hbm, gain_ref, wo_hbm, wg_hbm, wu_hbm, wd_hbm, out_hbm,
         xh, att, h, part, got, send, cross, b, act, wo, wg, wu, wd, lsem, osem, msem, csem, fsem) = refs
    else:
        (x_hbm, att_hbm, gain_ref, wo_hbm, wg_hbm, wu_hbm, wd_hbm, next_gain_ref, cos_ref, sin_ref, wq_hbm, wk_hbm, wv_hbm, out_hbm, q_ref, k_ref, v_ref,
         xh, att, h, part, got, send, cross, b, act, wo, wg, wu, wd, wq, wk, wv, lsem, osem, msem, csem, fsem) = refs
    tp = lax.axis_index('tp')
    core = lax.rem(tp, 2)
    mate = tp + 1 - 2 * core
    peer = lax.rem(tp + 2, 4)
    half = h.shape[2]
    own_cols = pl.ds(pl.multiple_of(core * half, half), half)

    loads = [(x_hbm.at[:, own_cols], xh), (att_hbm, att), (wo_hbm.at[layer], wo), (wg_hbm.at[layer], wg), (wu_hbm.at[layer], wu), (wd_hbm.at[layer], wd)]
    if not last:
        loads += [(wq_hbm.at[layer + 1], wq), (wk_hbm.at[layer + 1], wk), (wv_hbm.at[layer + 1], wv)]
    loads = [pltpu.make_async_copy(src, dst, lsem.at[n]) for n, (src, dst) in enumerate(loads)]
    order = [1, 2, 0, 3, 4, 5] + list(range(6, len(loads)))
    for n in order:
        loads[n].start()

    barrier = pltpu.get_barrier_semaphore()
    for other in (mate, peer):
        pl.semaphore_signal(barrier, inc=1, device_id={'tp': other}, device_id_type=MESH)
    pl.semaphore_wait(barrier, 2)

    def remote(src, dst, sem, idx, device):
        return pltpu.make_async_remote_copy(src_ref=src, dst_ref=dst, send_sem=sem.at[0, idx[0], idx[1]], recv_sem=sem.at[1, idx[0], idx[1]], device_id={'tp': device}, device_id_type=MESH)

    def to_mate(phase, g):
        at = pl.ds(*groups[g])
        return remote(part.at[1 - core, at], got.at[at], msem, (phase, g), mate)

    def to_peer(phase, g):
        at = pl.ds(*groups[g])
        return remote(send.at[at], cross.at[phase, at], csem, (phase, g), peer)

    def final(phase, g):
        at = pl.ds(*groups[g])
        return remote(h.at[core, at], h.at[core, at], fsem, (phase, g), mate)

    def project(lhs_ref, lhs_at, w_ref, g):
        row0, rows = groups[g]
        per_half = half // TILE

        def tile(j, _):
            col = pl.multiple_of(j * TILE, TILE)
            prod = jnp.dot(lhs_ref[lhs_at, :], w_ref[:, pl.ds(col, TILE)], preferred_element_type=F32)
            side = j // per_half
            part[side, pl.ds(row0, rows), pl.ds(pl.multiple_of((j - side * per_half) * TILE, TILE), TILE)] = prod.astype(BF16)
            return 0

        lax.fori_loop(0, 2 * per_half, tile, 0)

    def chip_sum(g):
        row0, rows = groups[g]

        def step(i, _):
            at = pl.ds(pl.multiple_of(row0 + i * 16, 16), 16)
            send[at, :] = (part[core, at, :].astype(F32) + got[at, :].astype(F32)).astype(BF16)
            return 0

        lax.fori_loop(0, rows // 16, step, 0)

    def add_sum(phase, base_ref, g):
        row0, rows = groups[g]

        def step(i, _):
            at = pl.ds(pl.multiple_of(row0 + i * 16, 16), 16)
            base = xh[at, :] if phase == 0 else h[core, at, :]
            total = send[at, :].astype(F32) + cross[phase, at, :].astype(F32)
            h[core, at, :] = (base.astype(F32) + total).astype(BF16)
            return 0

        lax.fori_loop(0, rows // 16, step, 0)

    loads[1].wait()
    loads[2].wait()
    for g in range(len(groups)):
        project(att, pl.ds(*groups[g]), wo, g)
        to_mate(0, g).start()
    loads[0].wait()
    for g in range(len(groups)):
        to_mate(0, g).wait()
        chip_sum(g)
        to_peer(0, g).start()
    for n in (3, 4, 5):
        loads[n].wait()
    mlp_gain = gain_ref[...].astype(F32)[layer:layer + 1, :]
    for g in range(len(groups)):
        rows = groups[g][1]
        to_peer(0, g).wait()
        add_sum(0, xh, g)
        final(0, g).start()
        final(0, g).wait()
        norm_rows(h, mlp_gain, b, groups[g][0], rows)

        def up_tile(j, _, rows=rows):
            cols = pl.ds(pl.multiple_of(j * TILE, TILE), TILE)
            gate = jnp.dot(b[0:rows, :], wg[:, cols], preferred_element_type=F32)
            up = jnp.dot(b[0:rows, :], wu[:, cols], preferred_element_type=F32)
            act[0:rows, cols] = (gate * (1.0 / (1.0 + jnp.exp(-gate))) * up).astype(BF16)
            return 0

        lax.fori_loop(0, wg.shape[1] // TILE, up_tile, 0)
        project(act, pl.ds(0, rows), wd, g)
        to_mate(1, g).start()
        to_mate(1, g).wait()
        chip_sum(g)
        to_peer(1, g).start()
    if not last:
        next_gain = next_gain_ref[...].astype(F32)[layer + 1:layer + 2, :]
        for n in (6, 7, 8):
            loads[n].wait()
    outs = []
    for g in range(len(groups)):
        row0, rows = groups[g]
        to_peer(1, g).wait()
        add_sum(1, None, g)
        final(1, g).start()
        final(1, g).wait()
        for s in range(2):
            outs.append(pltpu.make_async_copy(h.at[s, pl.ds(row0, rows)], out_hbm.at[pl.ds(row0, rows), pl.ds(s * half, half)], osem.at[g, s]))
            outs[-1].start()
        if not last:
            norm_rows(h, next_gain, b, row0, rows)
            qkv_rows(b, wq, wk, wv, cos_ref, sin_ref, q_ref, k_ref, v_ref, row0, rows)
    for copy in outs:
        copy.wait()


def block_call(layer, last, x, att, mlp_gain, w_o, w_gate, w_up, w_down, extra):
    rows, width = x.shape
    half = width // 2
    most = max(n for _, n in GROUPS)
    count = len(GROUPS)
    vmem = pl.BlockSpec(memory_space=pltpu.VMEM)
    hbm = pl.BlockSpec(memory_space=pl.ANY)
    out_shape = [jax.ShapeDtypeStruct((rows, width), BF16)]
    in_specs = [hbm, hbm, vmem, hbm, hbm, hbm, hbm]
    out_specs = [hbm]
    weights = [w_o, w_gate, w_up, w_down]
    if not last:
        in_specs += [vmem, vmem, vmem, hbm, hbm, hbm]
        weights += list(extra[3:])
        out_shape += [jax.ShapeDtypeStruct((rows, w.shape[2]), BF16) for w in extra[3:]]
        out_specs += [vmem] * 3
    return pl.pallas_call(
        functools.partial(block_kernel, layer, last, GROUPS),
        name=f'block_{layer}',
        out_shape=out_shape,
        in_specs=in_specs,
        out_specs=out_specs,
        scratch_shapes=[
            pltpu.VMEM((rows, half), BF16),
            pltpu.VMEM(att.shape, BF16),
            pltpu.VMEM((2, rows, half), BF16),
            pltpu.VMEM((2, rows, half), BF16),
            pltpu.VMEM((rows, half), BF16),
            pltpu.VMEM((rows, half), BF16),
            pltpu.VMEM((2, rows, half), BF16),
            pltpu.VMEM((most, width), BF16),
            pltpu.VMEM((most, w_down.shape[1]), BF16),
        ] + [pltpu.VMEM(w.shape[1:], BF16) for w in weights] + [
            pltpu.SemaphoreType.DMA((9,)),
            pltpu.SemaphoreType.DMA((count, 2)),
            pltpu.SemaphoreType.DMA((2, 2, count)),
            pltpu.SemaphoreType.DMA((2, 2, count)),
            pltpu.SemaphoreType.DMA((2, 2, count)),
        ],
        compiler_params=pltpu.CompilerParams(collective_id=layer, has_side_effects=True, vmem_limit_bytes=VMEM_LIMIT),
    )(x, att, mlp_gain, w_o, w_gate, w_up, w_down, *extra)


def solution(mesh):
    col_spec = P(None, None, 'tp')
    row_spec = P(None, 'tp', None)
    cache_spec = P(None, 'dp', 'tp', None, None)
    in_specs = (P('dp', None), P('dp'), P(), col_spec, col_spec, col_spec, row_spec, P(), col_spec, col_spec, row_spec, cache_spec, cache_spec)

    def body(x, lengths, attn_gain, w_q, w_k, w_v, w_o, mlp_gain, w_gate, w_up, w_down, k_cache, v_cache):
        dec_rows = lengths.shape[0] - 1
        chunk_len = x.shape[0] - dec_rows
        layers = w_q.shape[0]
        positions = jnp.concatenate([lengths[:dec_rows], lengths[dec_rows] + jnp.arange(chunk_len, dtype=jnp.int32)])
        cos, sin = rope_tables(positions, k_cache.shape[-1])
        q, k, v = qkv_call(x, attn_gain, cos, sin, w_q, w_k, w_v)
        for layer in range(layers):
            last = layer == layers - 1
            att = attention_call(layer, lengths, q, k, v, k_cache, v_cache)
            extra = () if last else (attn_gain, cos, sin, w_q, w_k, w_v)
            x, *rest = block_call(layer, last, x, att, mlp_gain, w_o, w_gate, w_up, w_down, extra)
            if not last:
                q, k, v = rest
        return x

    return jax.shard_map(body, mesh=mesh, in_specs=in_specs, out_specs=P('dp', None), check_vma=False)
```

```python
import functools

import jax
import jax.numpy as jnp
from jax import lax
from jax.experimental import pallas as pl
from jax.experimental.pallas import tpu as pltpu
from jax.sharding import PartitionSpec as P

ROPE_BASE = 500000.0
EPSILON = 1e-5
MESH = pl.DeviceIdType.MESH
F32 = jnp.float32
BF16 = jnp.bfloat16
VMEM_LIMIT = 64_600_000
TILE = 256
DOWN_TILE = 512
SLOTS = 3
GROUPS = ((0, 112), (112, 112), (224, 96))


def rope_tables(positions, head_dim):
    freq_exps = jnp.arange(0, head_dim, 2, dtype=F32) / head_dim
    angles = positions.astype(F32)[:, None] * jnp.power(ROPE_BASE, -freq_exps)[None, :]
    cos_half, sin_half = jnp.cos(angles), jnp.sin(angles)
    return jnp.concatenate([cos_half, cos_half], axis=-1), jnp.concatenate([-sin_half, sin_half], axis=-1)


def norm_rows(h_ref, gain, b_ref, row0, rows, block=16):
    half = h_ref.shape[2]
    gain_lo, gain_hi = gain[:, :half], gain[:, half:]

    def step(i, _):
        src = pl.ds(pl.multiple_of(row0 + i * block, block), block)
        dst = pl.ds(pl.multiple_of(i * block, block), block)
        lo, hi = h_ref[0, src, :].astype(F32), h_ref[1, src, :].astype(F32)
        total = jnp.sum(lo * lo, axis=-1, keepdims=True) + jnp.sum(hi * hi, axis=-1, keepdims=True)
        inv = lax.rsqrt(total / (2 * half) + EPSILON)
        b_ref[dst, :half] = (lo * inv * gain_lo).astype(BF16)
        b_ref[dst, half:] = (hi * inv * gain_hi).astype(BF16)
        return 0

    lax.fori_loop(0, rows // block, step, 0)


def rope_store(prod, cos, sin, out_ref, rows, col):
    head = cos.shape[1]
    for k in range(prod.shape[1] // head):
        vec = prod[:, k * head:(k + 1) * head].astype(BF16).astype(F32)
        rot = vec * cos + pltpu.roll(vec, head // 2, 1) * sin
        out_ref[rows, pl.ds(col + k * head, head)] = rot.astype(BF16)


def qkv_rows(b_ref, wq_ref, wk_ref, wv_ref, cos_ref, sin_ref, q_ref, k_ref, v_ref, row0, rows):
    rows_at = pl.ds(row0, rows)
    lhs = b_ref[0:rows, :]
    cos, sin = cos_ref[rows_at, :], sin_ref[rows_at, :]

    def q_tile(j, _):
        col = pl.multiple_of(j * TILE, TILE)
        prod = jnp.dot(b_ref[0:rows, :], wq_ref[:, pl.ds(col, TILE)], preferred_element_type=F32)
        rope_store(prod, cos_ref[rows_at, :], sin_ref[rows_at, :], q_ref, rows_at, col)
        return 0

    lax.fori_loop(0, wq_ref.shape[1] // TILE, q_tile, 0)
    rope_store(jnp.dot(lhs, wk_ref[...], preferred_element_type=F32), cos, sin, k_ref, rows_at, 0)
    v_ref[rows_at, :] = jnp.dot(lhs, wv_ref[...], preferred_element_type=F32).astype(BF16)


def qkv_kernel(x_hbm, gain_ref, cos_ref, sin_ref, wq_hbm, wk_hbm, wv_hbm, q_ref, k_ref, v_ref, h, b, wq, wk, wv, sems):
    half = h.shape[2]
    copies = [pltpu.make_async_copy(x_hbm.at[:, pl.ds(s * half, half)], h.at[s], sems.at[s]) for s in range(2)]
    copies += [pltpu.make_async_copy(src.at[0], dst, sems.at[2 + n]) for n, (src, dst) in enumerate(((wq_hbm, wq), (wk_hbm, wk), (wv_hbm, wv)))]
    for copy in copies:
        copy.start()
    copies[0].wait()
    copies[1].wait()
    rows = h.shape[1]
    norm_rows(h, gain_ref[...].astype(F32)[0:1, :], b, 0, rows)
    for copy in copies[2:]:
        copy.wait()
    qkv_rows(b, wq, wk, wv, cos_ref, sin_ref, q_ref, k_ref, v_ref, 0, rows)


def qkv_call(x, gain, cos, sin, w_q, w_k, w_v):
    rows, width = x.shape
    vmem = pl.BlockSpec(memory_space=pltpu.VMEM)
    hbm = pl.BlockSpec(memory_space=pl.ANY)
    return pl.pallas_call(
        qkv_kernel,
        name='qkv_first',
        out_shape=[jax.ShapeDtypeStruct((rows, w.shape[2]), BF16) for w in (w_q, w_k, w_v)],
        in_specs=[hbm, vmem, vmem, vmem, hbm, hbm, hbm],
        out_specs=[vmem] * 3,
        scratch_shapes=[
            pltpu.VMEM((2, rows, width // 2), BF16),
            pltpu.VMEM((rows, width), BF16),
            pltpu.VMEM(w_q.shape[1:], BF16),
            pltpu.VMEM(w_k.shape[1:], BF16),
            pltpu.VMEM(w_v.shape[1:], BF16),
            pltpu.SemaphoreType.DMA((5,)),
        ],
        compiler_params=pltpu.CompilerParams(vmem_limit_bytes=61 * 2**20),
    )(x, gain, cos, sin, w_q, w_k, w_v)


UNIT = 128
BATCH = 8
BITS = (8, 4, 2, 1)


def attention_kernel(layer, len_ref, q_ref, k_ref, v_ref, kc_hbm, vc_hbm, o_ref, kbuf, vbuf, qs, kf, vf, sc, od, kp, vp, sems, psems):
    rows = kc_hbm.shape[1] - 1
    seq, head = kc_hbm.shape[3], kc_hbm.shape[4]
    heads = q_ref.shape[1] // head
    kv = kc_hbm.shape[2]
    rep = heads // kv
    chunk = q_ref.shape[0] - rows
    scale = head ** -0.5
    steps = rows // BATCH

    def copies(step, slot, act):
        for i in range(BATCH):
            row = step * BATCH + i
            units = (len_ref[row] + UNIT - 1) // UNIT
            for n, bit in enumerate(BITS):
                @pl.when((units // bit) % 2 == 1)
                def _(i=i, row=row, units=units, n=n, bit=bit):
                    off = pl.multiple_of((units // (2 * bit)) * (2 * bit * UNIT), UNIT)
                    span = pl.ds(off, bit * UNIT)
                    for m, (src, dst) in enumerate(((kc_hbm, kbuf), (vc_hbm, vbuf))):
                        copy = pltpu.make_async_copy(src.at[layer, row, :, span, :], dst.at[slot, i, :, span, :], sems.at[slot, i, n, m])
                        if act == 'start':
                            copy.start()
                        else:
                            copy.wait()

    prefill = [pltpu.make_async_copy(src.at[layer, rows], dst, psems.at[n]) for n, (src, dst) in enumerate(((kc_hbm, kp), (vc_hbm, vp)))]
    for copy in prefill:
        copy.start()

    for slot in range(SLOTS):
        def clear(i, _, slot=slot):
            for g in range(kv):
                vbuf[slot, i, g] = jnp.zeros((seq, head), BF16)
            return 0

        lax.fori_loop(0, BATCH, clear, 0)
        if slot < SLOTS - 1:
            copies(slot, slot, 'start')

    qs[...] = jnp.zeros_like(qs)
    for h in range(heads):
        qs[h // rep, pl.ds(h, rows, stride=8), :] = q_ref[0:rows, h * head:(h + 1) * head].astype(F32)
    kf[...] = k_ref[0:rows, :].astype(F32)
    vf[...] = v_ref[0:rows, :].astype(F32)

    for copy in prefill:
        copy.wait()
    limit = len_ref[rows]

    def prefill_head(h, _):
        g = h // rep
        q = q_ref[rows:, pl.ds(pl.multiple_of(h * head, head), head)]
        kn = k_ref[rows:, pl.ds(pl.multiple_of(g * head, head), head)]
        vn = v_ref[rows:, pl.ds(pl.multiple_of(g * head, head), head)]
        dims = (((1,), (1,)), ((), ()))
        s_old = lax.dot_general(q, kp[g], dims, preferred_element_type=F32) * scale
        s_new = lax.dot_general(q, kn, dims, preferred_element_type=F32) * scale
        s_old = jnp.where(lax.broadcasted_iota(jnp.int32, s_old.shape, 1) < limit, s_old, -jnp.inf)
        causal = lax.broadcasted_iota(jnp.int32, s_new.shape, 1) <= lax.broadcasted_iota(jnp.int32, s_new.shape, 0)
        s_new = jnp.where(causal, s_new, -jnp.inf)
        top = jnp.maximum(jnp.max(s_old, axis=-1, keepdims=True), jnp.max(s_new, axis=-1, keepdims=True))
        e_old, e_new = jnp.exp(s_old - top), jnp.exp(s_new - top)
        inv = 1.0 / (jnp.sum(e_old, axis=-1, keepdims=True) + jnp.sum(e_new, axis=-1, keepdims=True))
        out = jnp.dot((e_old * inv).astype(BF16), vp[g], preferred_element_type=F32)
        out += jnp.dot((e_new * inv).astype(BF16), vn, preferred_element_type=F32)
        o_ref[rows:, pl.ds(pl.multiple_of(h * head, head), head)] = out.astype(BF16)
        return 0

    lax.fori_loop(0, heads, prefill_head, 0)

    def decode_step(step, _):
        slot = lax.rem(step, SLOTS)

        @pl.when(step + SLOTS - 1 < steps)
        def _():
            copies(step + SLOTS - 1, lax.rem(step + SLOTS - 1, SLOTS), 'start')

        copies(step, slot, 'wait')
        for i in range(BATCH):
            row = step * BATCH + i
            length = len_ref[row]
            base = pl.multiple_of((length // 16) * 16, 16)
            hit = lax.broadcasted_iota(jnp.int32, (16, head), 0) == length - base
            for buf, new in ((kbuf, kf), (vbuf, vf)):
                for g in range(kv):
                    old = buf[slot, i, g, pl.ds(base, 16), :].astype(F32)
                    mine = new[pl.ds(pl.multiple_of(step * BATCH, BATCH), BATCH), g * head:(g + 1) * head][i:i + 1, :]
                    buf[slot, i, g, pl.ds(base, 16), :] = jnp.where(hit, mine, old).astype(BF16)
        for i in range(BATCH):
            row = step * BATCH + i
            at = pl.ds(pl.multiple_of(row * 8, 8), 8)
            q = jnp.concatenate([qs[g, at, :] for g in range(kv)], axis=-1).astype(BF16)
            keys = jnp.concatenate([kbuf[slot, i, g] for g in range(kv)], axis=-1)
            s = lax.dot_general(q, keys, (((1,), (1,)), ((), ())), preferred_element_type=F32) * scale
            s = jnp.where(lax.broadcasted_iota(jnp.int32, s.shape, 1) <= len_ref[row], s, -jnp.inf)
            sc[i * 8:(i + 1) * 8, :] = s
        for i in range(BATCH):
            s = sc[i * 8:(i + 1) * 8, :]
            e = jnp.exp(s - jnp.max(s, axis=-1, keepdims=True))
            p = (e * (1.0 / jnp.sum(e, axis=-1, keepdims=True))).astype(BF16)
            values = jnp.concatenate([vbuf[slot, i, g] for g in range(kv)], axis=-1)
            o = jnp.dot(p, values, preferred_element_type=F32)
            own = lax.broadcasted_iota(jnp.int32, (8, head), 0) // rep
            pick = o[:, 0:head]
            for g in range(1, kv):
                pick = jnp.where(own == g, o[:, g * head:(g + 1) * head], pick)
            row = step * BATCH + i
            od[pl.ds(pl.multiple_of(row * 8, 8), 8), :] = pick
        return 0

    lax.fori_loop(0, steps, decode_step, 0)
    for h in range(heads):
        o_ref[0:rows, h * head:(h + 1) * head] = od[pl.ds(h, rows, stride=8), :].astype(BF16)


def attention_call(layer, lengths, q, k, v, k_cache, v_cache):
    rows = k_cache.shape[1] - 1
    kv, seq, head = k_cache.shape[2:]
    vmem = pl.BlockSpec(memory_space=pltpu.VMEM)
    hbm = pl.BlockSpec(memory_space=pl.ANY)
    return pl.pallas_call(
        functools.partial(attention_kernel, layer),
        name=f'attention_{layer}',
        out_shape=jax.ShapeDtypeStruct(q.shape, BF16),
        in_specs=[pl.BlockSpec(memory_space=pltpu.SMEM), vmem, vmem, vmem, hbm, hbm],
        out_specs=vmem,
        scratch_shapes=[
            pltpu.VMEM((SLOTS, BATCH, kv, seq, head), BF16),
            pltpu.VMEM((SLOTS, BATCH, kv, seq, head), BF16),
            pltpu.VMEM((kv, rows * 8, head), F32),
            pltpu.VMEM((rows, kv * head), F32),
            pltpu.VMEM((rows, kv * head), F32),
            pltpu.VMEM((BATCH * 8, seq), F32),
            pltpu.VMEM((rows * 8, head), F32),
            pltpu.VMEM((kv, seq, head), BF16),
            pltpu.VMEM((kv, seq, head), BF16),
            pltpu.SemaphoreType.DMA((SLOTS, BATCH, len(BITS), 2)),
            pltpu.SemaphoreType.DMA((2,)),
        ],
        compiler_params=pltpu.CompilerParams(vmem_limit_bytes=60 * 2**20),
    )(lengths, q, k, v, k_cache, v_cache)


def block_kernel(layer, last, groups, *refs):
    if last:
        (x_hbm, att, gain_ref, wo_hbm, wg_hbm, wu_hbm, wd_hbm, out_hbm,
         xh, h, part, got, send, cross, b, act, wo, wg, wu, wd, lsem, osem, msem, csem, fsem) = refs
    else:
        (x_hbm, att, gain_ref, wo_hbm, wg_hbm, wu_hbm, wd_hbm, next_gain_ref, cos_ref, sin_ref, wq_hbm, wk_hbm, wv_hbm, out_hbm, q_ref, k_ref, v_ref,
         xh, h, part, got, send, cross, b, act, wo, wg, wu, wd, wq, wk, wv, lsem, osem, msem, csem, fsem) = refs
    tp = lax.axis_index('tp')
    core = lax.rem(tp, 2)
    mate = tp + 1 - 2 * core
    peer = lax.rem(tp + 2, 4)
    half = h.shape[2]
    own_cols = pl.ds(pl.multiple_of(core * half, half), half)

    loads = [(x_hbm.at[:, own_cols], xh), (wo_hbm.at[layer], wo), (wg_hbm.at[layer], wg), (wu_hbm.at[layer], wu), (wd_hbm.at[layer], wd)]
    if not last:
        loads += [(wq_hbm.at[layer + 1], wq), (wk_hbm.at[layer + 1], wk), (wv_hbm.at[layer + 1], wv)]
    loads = [pltpu.make_async_copy(src, dst, lsem.at[n]) for n, (src, dst) in enumerate(loads)]
    order = [1, 0] + list(range(2, len(loads)))
    for n in order:
        loads[n].start()

    barrier = pltpu.get_barrier_semaphore()
    for other in (mate, peer):
        pl.semaphore_signal(barrier, inc=1, device_id={'tp': other}, device_id_type=MESH)
    pl.semaphore_wait(barrier, 2)

    def remote(src, dst, sem, idx, device):
        return pltpu.make_async_remote_copy(src_ref=src, dst_ref=dst, send_sem=sem.at[0, idx[0], idx[1]], recv_sem=sem.at[1, idx[0], idx[1]], device_id={'tp': device}, device_id_type=MESH)

    def to_mate(phase, g):
        at = pl.ds(*groups[g])
        return remote(part.at[1 - core, at], got.at[at], msem, (phase, g), mate)

    def to_peer(phase, g):
        at = pl.ds(*groups[g])
        return remote(send.at[at], cross.at[phase, at], csem, (phase, g), peer)

    def final(phase, g):
        at = pl.ds(*groups[g])
        return remote(h.at[core, at], h.at[core, at], fsem, (phase, g), mate)

    def project(lhs_ref, lhs_at, w_ref, g):
        row0, rows = groups[g]
        per_half = half // DOWN_TILE

        def tile(j, _):
            col = pl.multiple_of(j * DOWN_TILE, DOWN_TILE)
            prod = jnp.dot(lhs_ref[lhs_at, :], w_ref[:, pl.ds(col, DOWN_TILE)], preferred_element_type=F32)
            side = j // per_half
            part[side, pl.ds(row0, rows), pl.ds(pl.multiple_of((j - side * per_half) * DOWN_TILE, DOWN_TILE), DOWN_TILE)] = prod.astype(BF16)
            return 0

        lax.fori_loop(0, 2 * per_half, tile, 0, unroll=2)

    def chip_sum(g):
        row0, rows = groups[g]

        def step(i, _):
            at = pl.ds(pl.multiple_of(row0 + i * 16, 16), 16)
            send[at, :] = (part[core, at, :].astype(F32) + got[at, :].astype(F32)).astype(BF16)
            return 0

        lax.fori_loop(0, rows // 16, step, 0)

    def add_sum(phase, g):
        row0, rows = groups[g]

        def step(i, _):
            at = pl.ds(pl.multiple_of(row0 + i * 16, 16), 16)
            base = xh[at, :] if phase == 0 else h[core, at, :]
            total = send[at, :].astype(F32) + cross[phase, at, :].astype(F32)
            h[core, at, :] = (base.astype(F32) + total).astype(BF16)
            return 0

        lax.fori_loop(0, rows // 16, step, 0)

    count = len(groups)

    def arrive(phase, g):
        to_peer(phase, g).wait()
        add_sum(phase, g)
        final(phase, g).start()

    def leave(phase, g):
        to_mate(phase, g).wait()
        chip_sum(g)
        to_peer(phase, g).start()

    loads[1].wait()
    for g in range(count):
        project(att, pl.ds(*groups[g]), wo, g)
        to_mate(0, g).start()
        if g > 0:
            leave(0, g - 1)
    leave(0, count - 1)
    loads[0].wait()
    mlp_gain = gain_ref[...].astype(F32)[layer:layer + 1, :]
    arrive(0, 0)
    for g in range(count):
        row0, rows = groups[g]
        final(0, g).wait()
        norm_rows(h, mlp_gain, b, row0, rows)
        if g == 0:
            loads[2].wait()
            loads[3].wait()

        def up_tile(j, _, rows=rows):
            cols = pl.ds(pl.multiple_of(j * TILE, TILE), TILE)
            gate = jnp.dot(b[0:rows, :], wg[:, cols], preferred_element_type=F32)
            up = jnp.dot(b[0:rows, :], wu[:, cols], preferred_element_type=F32)
            act[0:rows, cols] = (gate * (1.0 / (1.0 + jnp.exp(-gate))) * up).astype(BF16)
            return 0

        lax.fori_loop(0, wg.shape[1] // TILE, up_tile, 0, unroll=2)
        if g == 0:
            loads[4].wait()
        project(act, pl.ds(0, rows), wd, g)
        to_mate(1, g).start()
        if g + 1 < count:
            arrive(0, g + 1)
        leave(1, g)
    if not last:
        next_gain = next_gain_ref[...].astype(F32)[layer + 1:layer + 2, :]
        for n in (5, 6, 7):
            loads[n].wait()
    outs = []
    for g in range(len(groups)):
        row0, rows = groups[g]
        arrive(1, g)
        final(1, g).wait()
        for s in range(2):
            outs.append(pltpu.make_async_copy(h.at[s, pl.ds(row0, rows)], out_hbm.at[pl.ds(row0, rows), pl.ds(s * half, half)], osem.at[g, s]))
            outs[-1].start()
        if not last:
            norm_rows(h, next_gain, b, row0, rows)
            qkv_rows(b, wq, wk, wv, cos_ref, sin_ref, q_ref, k_ref, v_ref, row0, rows)
    for copy in outs:
        copy.wait()


def block_call(layer, last, x, att, mlp_gain, w_o, w_gate, w_up, w_down, extra):
    rows, width = x.shape
    half = width // 2
    most = max(n for _, n in GROUPS)
    count = len(GROUPS)
    vmem = pl.BlockSpec(memory_space=pltpu.VMEM)
    hbm = pl.BlockSpec(memory_space=pl.ANY)
    out_shape = [jax.ShapeDtypeStruct((rows, width), BF16)]
    in_specs = [hbm, vmem, vmem, hbm, hbm, hbm, hbm]
    out_specs = [hbm]
    weights = [w_o, w_gate, w_up, w_down]
    if not last:
        in_specs += [vmem, vmem, vmem, hbm, hbm, hbm]
        weights += list(extra[3:])
        out_shape += [jax.ShapeDtypeStruct((rows, w.shape[2]), BF16) for w in extra[3:]]
        out_specs += [vmem] * 3
    return pl.pallas_call(
        functools.partial(block_kernel, layer, last, GROUPS),
        name=f'block_{layer}',
        out_shape=out_shape,
        in_specs=in_specs,
        out_specs=out_specs,
        scratch_shapes=[
            pltpu.VMEM((rows, half), BF16),
            pltpu.VMEM((2, rows, half), BF16),
            pltpu.VMEM((2, rows, half), BF16),
            pltpu.VMEM((rows, half), BF16),
            pltpu.VMEM((rows, half), BF16),
            pltpu.VMEM((2, rows, half), BF16),
            pltpu.VMEM((most, width), BF16),
            pltpu.VMEM((most, w_down.shape[1]), BF16),
        ] + [pltpu.VMEM(w.shape[1:], BF16) for w in weights] + [
            pltpu.SemaphoreType.DMA((8,)),
            pltpu.SemaphoreType.DMA((count, 2)),
            pltpu.SemaphoreType.DMA((2, 2, count)),
            pltpu.SemaphoreType.DMA((2, 2, count)),
            pltpu.SemaphoreType.DMA((2, 2, count)),
        ],
        compiler_params=pltpu.CompilerParams(collective_id=layer, has_side_effects=True, vmem_limit_bytes=VMEM_LIMIT),
    )(x, att, mlp_gain, w_o, w_gate, w_up, w_down, *extra)


def solution(mesh):
    col_spec = P(None, None, 'tp')
    row_spec = P(None, 'tp', None)
    cache_spec = P(None, 'dp', 'tp', None, None)
    in_specs = (P('dp', None), P('dp'), P(), col_spec, col_spec, col_spec, row_spec, P(), col_spec, col_spec, row_spec, cache_spec, cache_spec)

    def body(x, lengths, attn_gain, w_q, w_k, w_v, w_o, mlp_gain, w_gate, w_up, w_down, k_cache, v_cache):
        dec_rows = lengths.shape[0] - 1
        chunk_len = x.shape[0] - dec_rows
        layers = w_q.shape[0]
        positions = jnp.concatenate([lengths[:dec_rows], lengths[dec_rows] + jnp.arange(chunk_len, dtype=jnp.int32)])
        cos, sin = rope_tables(positions, k_cache.shape[-1])
        q, k, v = qkv_call(x, attn_gain, cos, sin, w_q, w_k, w_v)
        for layer in range(layers):
            last = layer == layers - 1
            att = attention_call(layer, lengths, q, k, v, k_cache, v_cache)
            extra = () if last else (attn_gain, cos, sin, w_q, w_k, w_v)
            x, *rest = block_call(layer, last, x, att, mlp_gain, w_o, w_gate, w_up, w_down, extra)
            if not last:
                q, k, v = rest
        return x

    return jax.shard_map(body, mesh=mesh, in_specs=in_specs, out_specs=P('dp', None), check_vma=False)
```

```python
import functools

import jax
import jax.numpy as jnp
from jax import lax
from jax.experimental import pallas as pl
from jax.experimental.pallas import tpu as pltpu
from jax.sharding import PartitionSpec as P

ROPE_BASE = 500000.0
EPSILON = 1e-5
MESH = pl.DeviceIdType.MESH
F32 = jnp.float32
BF16 = jnp.bfloat16
VMEM_LIMIT = 64_600_000
TILE = 256
DOWN_TILE = 512
SLOTS = 3
GROUPS = ((0, 112), (112, 112), (224, 96))


def rope_tables(positions, head_dim):
    freq_exps = jnp.arange(0, head_dim, 2, dtype=F32) / head_dim
    angles = positions.astype(F32)[:, None] * jnp.power(ROPE_BASE, -freq_exps)[None, :]
    cos_half, sin_half = jnp.cos(angles), jnp.sin(angles)
    return jnp.concatenate([cos_half, cos_half], axis=-1), jnp.concatenate([-sin_half, sin_half], axis=-1)


def norm_rows(h_ref, gain, b_ref, row0, rows, block=16):
    half = h_ref.shape[2]
    gain_lo, gain_hi = gain[:, :half], gain[:, half:]

    def step(i, _):
        src = pl.ds(pl.multiple_of(row0 + i * block, block), block)
        dst = pl.ds(pl.multiple_of(i * block, block), block)
        lo, hi = h_ref[0, src, :].astype(F32), h_ref[1, src, :].astype(F32)
        total = jnp.sum(lo * lo, axis=-1, keepdims=True) + jnp.sum(hi * hi, axis=-1, keepdims=True)
        inv = lax.rsqrt(total / (2 * half) + EPSILON)
        b_ref[dst, :half] = (lo * inv * gain_lo).astype(BF16)
        b_ref[dst, half:] = (hi * inv * gain_hi).astype(BF16)
        return 0

    lax.fori_loop(0, rows // block, step, 0)


def rope_store(prod, cos, sin, out_ref, rows, col):
    head = cos.shape[1]
    for k in range(prod.shape[1] // head):
        vec = prod[:, k * head:(k + 1) * head].astype(BF16).astype(F32)
        rot = vec * cos + pltpu.roll(vec, head // 2, 1) * sin
        out_ref[rows, pl.ds(col + k * head, head)] = rot.astype(BF16)


def qkv_rows(b_ref, wq_ref, wk_ref, wv_ref, cos_ref, sin_ref, q_ref, k_ref, v_ref, row0, rows):
    rows_at = pl.ds(row0, rows)
    lhs = b_ref[0:rows, :]
    cos, sin = cos_ref[rows_at, :], sin_ref[rows_at, :]

    def q_tile(j, _):
        col = pl.multiple_of(j * TILE, TILE)
        prod = jnp.dot(b_ref[0:rows, :], wq_ref[:, pl.ds(col, TILE)], preferred_element_type=F32)
        rope_store(prod, cos_ref[rows_at, :], sin_ref[rows_at, :], q_ref, rows_at, col)
        return 0

    lax.fori_loop(0, wq_ref.shape[1] // TILE, q_tile, 0)
    rope_store(jnp.dot(lhs, wk_ref[...], preferred_element_type=F32), cos, sin, k_ref, rows_at, 0)
    v_ref[rows_at, :] = jnp.dot(lhs, wv_ref[...], preferred_element_type=F32).astype(BF16)


def qkv_kernel(x_hbm, gain_ref, cos_ref, sin_ref, wq_hbm, wk_hbm, wv_hbm, q_ref, k_ref, v_ref, h, b, wq, wk, wv, sems):
    half = h.shape[2]
    copies = [pltpu.make_async_copy(x_hbm.at[:, pl.ds(s * half, half)], h.at[s], sems.at[s]) for s in range(2)]
    copies += [pltpu.make_async_copy(src.at[0], dst, sems.at[2 + n]) for n, (src, dst) in enumerate(((wq_hbm, wq), (wk_hbm, wk), (wv_hbm, wv)))]
    for copy in copies:
        copy.start()
    copies[0].wait()
    copies[1].wait()
    rows = h.shape[1]
    norm_rows(h, gain_ref[...].astype(F32)[0:1, :], b, 0, rows)
    for copy in copies[2:]:
        copy.wait()
    qkv_rows(b, wq, wk, wv, cos_ref, sin_ref, q_ref, k_ref, v_ref, 0, rows)


def qkv_call(x, gain, cos, sin, w_q, w_k, w_v):
    rows, width = x.shape
    vmem = pl.BlockSpec(memory_space=pltpu.VMEM)
    hbm = pl.BlockSpec(memory_space=pl.ANY)
    return pl.pallas_call(
        qkv_kernel,
        name='qkv_first',
        out_shape=[jax.ShapeDtypeStruct((rows, w.shape[2]), BF16) for w in (w_q, w_k, w_v)],
        in_specs=[hbm, vmem, vmem, vmem, hbm, hbm, hbm],
        out_specs=[vmem] * 3,
        scratch_shapes=[
            pltpu.VMEM((2, rows, width // 2), BF16),
            pltpu.VMEM((rows, width), BF16),
            pltpu.VMEM(w_q.shape[1:], BF16),
            pltpu.VMEM(w_k.shape[1:], BF16),
            pltpu.VMEM(w_v.shape[1:], BF16),
            pltpu.SemaphoreType.DMA((5,)),
        ],
        compiler_params=pltpu.CompilerParams(vmem_limit_bytes=61 * 2**20),
    )(x, gain, cos, sin, w_q, w_k, w_v)


BATCH = 8
SPAN = 256


def length_order(lengths):
    ids = jnp.arange(lengths.shape[0], dtype=jnp.int32)
    mine, other = lengths[:, None], lengths[None, :]
    ahead = (other > mine) | ((other == mine) & (ids[None, :] < ids[:, None]))
    rank = jnp.sum(ahead.astype(jnp.int32), axis=1)
    return jnp.sum(jnp.where(rank[None, :] == ids[:, None], ids[None, :], 0), axis=1)


def attention_kernel(layer, len_ref, order_ref, q_ref, k_ref, v_ref, kc_hbm, vc_hbm, o_ref, kbuf, vbuf, qs, kf, vf, sc, od, kp, vp, sems, psems):
    rows = kc_hbm.shape[1] - 1
    seq, head = kc_hbm.shape[3], kc_hbm.shape[4]
    heads = q_ref.shape[1] // head
    kv = kc_hbm.shape[2]
    rep = heads // kv
    scale = head ** -0.5
    steps = rows // BATCH
    spans = seq // SPAN
    nt = (((1,), (1,)), ((), ()))

    def step_spans(step):
        return len_ref[order_ref[step * BATCH]] // SPAN + 1

    def copies(step, slot, n, act):
        at = pl.ds(0, n * SPAN)
        for i in range(BATCH):
            row = order_ref[step * BATCH + i]
            for m, (src, dst) in enumerate(((kc_hbm, kbuf), (vc_hbm, vbuf))):
                copy = pltpu.make_async_copy(src.at[layer, row, :, at, :], dst.at[slot, i, :, at, :], sems.at[slot, i, m])
                if act == 'start':
                    copy.start()
                else:
                    copy.wait()

    def fetch(step, slot):
        for n in range(1, spans + 1):
            @pl.when(step_spans(step) == n)
            def _(n=n):
                copies(step, slot, n, 'start')

    prefill = [pltpu.make_async_copy(src.at[layer, rows], dst, psems.at[n]) for n, (src, dst) in enumerate(((kc_hbm, kp), (vc_hbm, vp)))]
    for copy in prefill:
        copy.start()
    for step in range(SLOTS - 1):
        fetch(step, step)

    qs[...] = jnp.zeros_like(qs)
    for h in range(heads):
        qs[h // rep, pl.ds(h, rows, stride=8), :] = q_ref[0:rows, h * head:(h + 1) * head].astype(F32)
    kf[...] = k_ref[0:rows, :].astype(F32)
    vf[...] = v_ref[0:rows, :].astype(F32)

    for copy in prefill:
        copy.wait()
    limit = len_ref[rows]

    def prefill_head(h, _, keys):
        g = h // rep
        q = q_ref[rows:, pl.ds(pl.multiple_of(h * head, head), head)]
        kn = k_ref[rows:, pl.ds(pl.multiple_of(g * head, head), head)]
        vn = v_ref[rows:, pl.ds(pl.multiple_of(g * head, head), head)]
        s_old = lax.dot_general(q, kp[g, 0:keys, :], nt, preferred_element_type=F32) * scale
        s_new = lax.dot_general(q, kn, nt, preferred_element_type=F32) * scale
        s_old = jnp.where(lax.broadcasted_iota(jnp.int32, s_old.shape, 1) < limit, s_old, -jnp.inf)
        causal = lax.broadcasted_iota(jnp.int32, s_new.shape, 1) <= lax.broadcasted_iota(jnp.int32, s_new.shape, 0)
        s_new = jnp.where(causal, s_new, -jnp.inf)
        top = jnp.maximum(jnp.max(s_old, axis=-1, keepdims=True), jnp.max(s_new, axis=-1, keepdims=True))
        e_old, e_new = jnp.exp(s_old - top), jnp.exp(s_new - top)
        inv = 1.0 / (jnp.sum(e_old, axis=-1, keepdims=True) + jnp.sum(e_new, axis=-1, keepdims=True))
        out = jnp.dot((e_old * inv).astype(BF16), vp[g, 0:keys, :], preferred_element_type=F32)
        out += jnp.dot((e_new * inv).astype(BF16), vn, preferred_element_type=F32)
        o_ref[rows:, pl.ds(pl.multiple_of(h * head, head), head)] = out.astype(BF16)
        return 0

    for n in range(1, spans + 1):
        @pl.when((limit + SPAN - 1) // SPAN == n)
        def _(n=n):
            lax.fori_loop(0, heads, functools.partial(prefill_head, keys=n * SPAN), 0)

    def attend(step, slot, n):
        keys = n * SPAN
        copies(step, slot, n, 'wait')
        for i in range(BATCH):
            row = order_ref[step * BATCH + i]
            length = len_ref[row]
            base = pl.multiple_of((length // 16) * 16, 16)
            hit = lax.broadcasted_iota(jnp.int32, (16, head), 0) == length - base
            near = pl.ds(pl.multiple_of((row // 8) * 8, 8), 8)
            pick = lax.broadcasted_iota(jnp.int32, (8, head), 0) == lax.rem(row, 8)
            for buf, new in ((kbuf, kf), (vbuf, vf)):
                for g in range(kv):
                    old = buf[slot, i, g, pl.ds(base, 16), :].astype(F32)
                    mine = jnp.sum(jnp.where(pick, new[near, g * head:(g + 1) * head], 0.0), axis=0, keepdims=True)
                    buf[slot, i, g, pl.ds(base, 16), :] = jnp.where(hit, mine, old).astype(BF16)
        for i in range(BATCH):
            row = order_ref[step * BATCH + i]
            at = pl.ds(pl.multiple_of(row * 8, 8), 8)
            q = jnp.concatenate([qs[g, at, :] for g in range(kv)], axis=-1).astype(BF16)
            key = jnp.concatenate([kbuf[slot, i, g, 0:keys, :] for g in range(kv)], axis=-1)
            s = lax.dot_general(q, key, nt, preferred_element_type=F32) * scale
            s = jnp.where(lax.broadcasted_iota(jnp.int32, s.shape, 1) <= len_ref[row], s, -jnp.inf)
            sc[i * 8:(i + 1) * 8, 0:keys] = s
        for i in range(BATCH):
            s = sc[i * 8:(i + 1) * 8, 0:keys]
            e = jnp.exp(s - jnp.max(s, axis=-1, keepdims=True))
            p = (e * (1.0 / jnp.sum(e, axis=-1, keepdims=True))).astype(BF16)
            value = jnp.concatenate([vbuf[slot, i, g, 0:keys, :] for g in range(kv)], axis=-1)
            o = jnp.dot(p, value, preferred_element_type=F32)
            own = lax.broadcasted_iota(jnp.int32, (8, head), 0) // rep
            pick = o[:, 0:head]
            for g in range(1, kv):
                pick = jnp.where(own == g, o[:, g * head:(g + 1) * head], pick)
            row = order_ref[step * BATCH + i]
            od[pl.ds(pl.multiple_of(row * 8, 8), 8), :] = pick

    def decode_step(step, _):
        slot = lax.rem(step, SLOTS)

        @pl.when(step + SLOTS - 1 < steps)
        def _():
            fetch(step + SLOTS - 1, lax.rem(step + SLOTS - 1, SLOTS))

        for n in range(1, spans + 1):
            @pl.when(step_spans(step) == n)
            def _(n=n):
                attend(step, slot, n)
        return 0

    lax.fori_loop(0, steps, decode_step, 0)
    for h in range(heads):
        o_ref[0:rows, h * head:(h + 1) * head] = od[pl.ds(h, rows, stride=8), :].astype(BF16)


def attention_call(layer, lengths, order, q, k, v, k_cache, v_cache):
    rows = k_cache.shape[1] - 1
    kv, seq, head = k_cache.shape[2:]
    vmem = pl.BlockSpec(memory_space=pltpu.VMEM)
    hbm = pl.BlockSpec(memory_space=pl.ANY)
    return pl.pallas_call(
        functools.partial(attention_kernel, layer),
        name=f'attention_{layer}',
        out_shape=jax.ShapeDtypeStruct(q.shape, BF16),
        in_specs=[pl.BlockSpec(memory_space=pltpu.SMEM)] * 2 + [vmem, vmem, vmem, hbm, hbm],
        out_specs=vmem,
        scratch_shapes=[
            pltpu.VMEM((SLOTS, BATCH, kv, seq, head), BF16),
            pltpu.VMEM((SLOTS, BATCH, kv, seq, head), BF16),
            pltpu.VMEM((kv, rows * 8, head), F32),
            pltpu.VMEM((rows, kv * head), F32),
            pltpu.VMEM((rows, kv * head), F32),
            pltpu.VMEM((BATCH * 8, seq), F32),
            pltpu.VMEM((rows * 8, head), F32),
            pltpu.VMEM((kv, seq, head), BF16),
            pltpu.VMEM((kv, seq, head), BF16),
            pltpu.SemaphoreType.DMA((SLOTS, BATCH, 2)),
            pltpu.SemaphoreType.DMA((2,)),
        ],
        compiler_params=pltpu.CompilerParams(vmem_limit_bytes=60 * 2**20),
    )(lengths, order, q, k, v, k_cache, v_cache)


def block_kernel(layer, last, groups, *refs):
    if last:
        (x_hbm, att, gain_ref, wo_hbm, wg_hbm, wu_hbm, wd_hbm, out_hbm,
         xh, h, part, got, send, cross, b, act, wo, wg, wu, wd, lsem, osem, msem, csem, fsem) = refs
    else:
        (x_hbm, att, gain_ref, wo_hbm, wg_hbm, wu_hbm, wd_hbm, next_gain_ref, cos_ref, sin_ref, wq_hbm, wk_hbm, wv_hbm, out_hbm, q_ref, k_ref, v_ref,
         xh, h, part, got, send, cross, b, act, wo, wg, wu, wd, wq, wk, wv, lsem, osem, msem, csem, fsem) = refs
    tp = lax.axis_index('tp')
    core = lax.rem(tp, 2)
    mate = tp + 1 - 2 * core
    peer = lax.rem(tp + 2, 4)
    half = h.shape[2]
    own_cols = pl.ds(pl.multiple_of(core * half, half), half)

    loads = [(x_hbm.at[:, own_cols], xh), (wo_hbm.at[layer], wo), (wg_hbm.at[layer], wg), (wu_hbm.at[layer], wu), (wd_hbm.at[layer], wd)]
    if not last:
        loads += [(wq_hbm.at[layer + 1], wq), (wk_hbm.at[layer + 1], wk), (wv_hbm.at[layer + 1], wv)]
    loads = [pltpu.make_async_copy(src, dst, lsem.at[n]) for n, (src, dst) in enumerate(loads)]
    order = [1, 0] + list(range(2, len(loads)))
    for n in order:
        loads[n].start()

    barrier = pltpu.get_barrier_semaphore()
    for other in (mate, peer):
        pl.semaphore_signal(barrier, inc=1, device_id={'tp': other}, device_id_type=MESH)
    pl.semaphore_wait(barrier, 2)

    def remote(src, dst, sem, idx, device):
        return pltpu.make_async_remote_copy(src_ref=src, dst_ref=dst, send_sem=sem.at[0, idx[0], idx[1]], recv_sem=sem.at[1, idx[0], idx[1]], device_id={'tp': device}, device_id_type=MESH)

    def to_mate(phase, g):
        at = pl.ds(*groups[g])
        return remote(part.at[1 - core, at], got.at[at], msem, (phase, g), mate)

    def to_peer(phase, g):
        at = pl.ds(*groups[g])
        return remote(send.at[at], cross.at[phase, at], csem, (phase, g), peer)

    def final(phase, g):
        at = pl.ds(*groups[g])
        return remote(h.at[core, at], h.at[core, at], fsem, (phase, g), mate)

    def project(lhs_ref, lhs_at, w_ref, g):
        row0, rows = groups[g]
        per_half = half // DOWN_TILE

        def tile(j, _):
            col = pl.multiple_of(j * DOWN_TILE, DOWN_TILE)
            prod = jnp.dot(lhs_ref[lhs_at, :], w_ref[:, pl.ds(col, DOWN_TILE)], preferred_element_type=F32)
            side = j // per_half
            part[side, pl.ds(row0, rows), pl.ds(pl.multiple_of((j - side * per_half) * DOWN_TILE, DOWN_TILE), DOWN_TILE)] = prod.astype(BF16)
            return 0

        lax.fori_loop(0, 2 * per_half, tile, 0, unroll=2)

    def chip_sum(g):
        row0, rows = groups[g]

        def step(i, _):
            at = pl.ds(pl.multiple_of(row0 + i * 16, 16), 16)
            send[at, :] = (part[core, at, :].astype(F32) + got[at, :].astype(F32)).astype(BF16)
            return 0

        lax.fori_loop(0, rows // 16, step, 0)

    def add_sum(phase, g):
        row0, rows = groups[g]

        def step(i, _):
            at = pl.ds(pl.multiple_of(row0 + i * 16, 16), 16)
            base = xh[at, :] if phase == 0 else h[core, at, :]
            total = send[at, :].astype(F32) + cross[phase, at, :].astype(F32)
            h[core, at, :] = (base.astype(F32) + total).astype(BF16)
            return 0

        lax.fori_loop(0, rows // 16, step, 0)

    count = len(groups)

    def arrive(phase, g):
        to_peer(phase, g).wait()
        add_sum(phase, g)
        final(phase, g).start()

    def leave(phase, g):
        to_mate(phase, g).wait()
        chip_sum(g)
        to_peer(phase, g).start()

    loads[1].wait()
    for g in range(count):
        project(att, pl.ds(*groups[g]), wo, g)
        to_mate(0, g).start()
        if g > 0:
            leave(0, g - 1)
    leave(0, count - 1)
    loads[0].wait()
    mlp_gain = gain_ref[...].astype(F32)[layer:layer + 1, :]
    arrive(0, 0)
    for g in range(count):
        row0, rows = groups[g]
        final(0, g).wait()
        norm_rows(h, mlp_gain, b, row0, rows)
        if g == 0:
            loads[2].wait()
            loads[3].wait()

        def up_tile(j, _, rows=rows):
            cols = pl.ds(pl.multiple_of(j * TILE, TILE), TILE)
            gate = jnp.dot(b[0:rows, :], wg[:, cols], preferred_element_type=F32)
            up = jnp.dot(b[0:rows, :], wu[:, cols], preferred_element_type=F32)
            act[0:rows, cols] = (gate * (1.0 / (1.0 + jnp.exp(-gate))) * up).astype(BF16)
            return 0

        lax.fori_loop(0, wg.shape[1] // TILE, up_tile, 0, unroll=2)
        if g == 0:
            loads[4].wait()
        project(act, pl.ds(0, rows), wd, g)
        to_mate(1, g).start()
        if g + 1 < count:
            arrive(0, g + 1)
        leave(1, g)
    if not last:
        next_gain = next_gain_ref[...].astype(F32)[layer + 1:layer + 2, :]
        for n in (5, 6, 7):
            loads[n].wait()
    outs = []
    for g in range(len(groups)):
        row0, rows = groups[g]
        arrive(1, g)
        final(1, g).wait()
        for s in range(2):
            outs.append(pltpu.make_async_copy(h.at[s, pl.ds(row0, rows)], out_hbm.at[pl.ds(row0, rows), pl.ds(s * half, half)], osem.at[g, s]))
            outs[-1].start()
        if not last:
            norm_rows(h, next_gain, b, row0, rows)
            qkv_rows(b, wq, wk, wv, cos_ref, sin_ref, q_ref, k_ref, v_ref, row0, rows)
    for copy in outs:
        copy.wait()


def block_call(layer, last, x, att, mlp_gain, w_o, w_gate, w_up, w_down, extra):
    rows, width = x.shape
    half = width // 2
    most = max(n for _, n in GROUPS)
    count = len(GROUPS)
    vmem = pl.BlockSpec(memory_space=pltpu.VMEM)
    hbm = pl.BlockSpec(memory_space=pl.ANY)
    out_shape = [jax.ShapeDtypeStruct((rows, width), BF16)]
    in_specs = [hbm, vmem, vmem, hbm, hbm, hbm, hbm]
    out_specs = [hbm]
    weights = [w_o, w_gate, w_up, w_down]
    if not last:
        in_specs += [vmem, vmem, vmem, hbm, hbm, hbm]
        weights += list(extra[3:])
        out_shape += [jax.ShapeDtypeStruct((rows, w.shape[2]), BF16) for w in extra[3:]]
        out_specs += [vmem] * 3
    return pl.pallas_call(
        functools.partial(block_kernel, layer, last, GROUPS),
        name=f'block_{layer}',
        out_shape=out_shape,
        in_specs=in_specs,
        out_specs=out_specs,
        scratch_shapes=[
            pltpu.VMEM((rows, half), BF16),
            pltpu.VMEM((2, rows, half), BF16),
            pltpu.VMEM((2, rows, half), BF16),
            pltpu.VMEM((rows, half), BF16),
            pltpu.VMEM((rows, half), BF16),
            pltpu.VMEM((2, rows, half), BF16),
            pltpu.VMEM((most, width), BF16),
            pltpu.VMEM((most, w_down.shape[1]), BF16),
        ] + [pltpu.VMEM(w.shape[1:], BF16) for w in weights] + [
            pltpu.SemaphoreType.DMA((8,)),
            pltpu.SemaphoreType.DMA((count, 2)),
            pltpu.SemaphoreType.DMA((2, 2, count)),
            pltpu.SemaphoreType.DMA((2, 2, count)),
            pltpu.SemaphoreType.DMA((2, 2, count)),
        ],
        compiler_params=pltpu.CompilerParams(collective_id=layer, has_side_effects=True, vmem_limit_bytes=VMEM_LIMIT),
    )(x, att, mlp_gain, w_o, w_gate, w_up, w_down, *extra)


def solution(mesh):
    col_spec = P(None, None, 'tp')
    row_spec = P(None, 'tp', None)
    cache_spec = P(None, 'dp', 'tp', None, None)
    in_specs = (P('dp', None), P('dp'), P(), col_spec, col_spec, col_spec, row_spec, P(), col_spec, col_spec, row_spec, cache_spec, cache_spec)

    def body(x, lengths, attn_gain, w_q, w_k, w_v, w_o, mlp_gain, w_gate, w_up, w_down, k_cache, v_cache):
        dec_rows = lengths.shape[0] - 1
        chunk_len = x.shape[0] - dec_rows
        layers = w_q.shape[0]
        positions = jnp.concatenate([lengths[:dec_rows], lengths[dec_rows] + jnp.arange(chunk_len, dtype=jnp.int32)])
        cos, sin = rope_tables(positions, k_cache.shape[-1])
        order = length_order(lengths[:dec_rows])
        q, k, v = qkv_call(x, attn_gain, cos, sin, w_q, w_k, w_v)
        for layer in range(layers):
            last = layer == layers - 1
            att = attention_call(layer, lengths, order, q, k, v, k_cache, v_cache)
            extra = () if last else (attn_gain, cos, sin, w_q, w_k, w_v)
            x, *rest = block_call(layer, last, x, att, mlp_gain, w_o, w_gate, w_up, w_down, extra)
            if not last:
                q, k, v = rest
        return x

    return jax.shard_map(body, mesh=mesh, in_specs=in_specs, out_specs=P('dp', None), check_vma=False)
```

```python
import functools
import math

import jax
import jax.numpy as jnp
from jax import lax
from jax.experimental import pallas as pl
from jax.experimental.pallas import tpu as pltpu
from jax.sharding import PartitionSpec as P

ROPE_BASE = 500000.0
EPSILON = 1e-5
MESH = pl.DeviceIdType.MESH
F32 = jnp.float32
BF16 = jnp.bfloat16
VMEM_LIMIT = 64_600_000
TILE = 256
DOWN_TILE = 512
SLOTS = 3
GROUPS = ((0, 112), (112, 112), (224, 96))


def rope_tables(len_ref, cos_ref, sin_ref):
    rows, head = cos_ref.shape
    dec_rows = len_ref.shape[0] - 1
    block = 8
    lane = lax.broadcasted_iota(jnp.int32, (block, head), 1)
    sub = lax.broadcasted_iota(jnp.int32, (block, head), 0)
    freq = jnp.exp(lax.rem(lane, head // 2).astype(F32) * (-2.0 / head * math.log(ROPE_BASE)))
    sign = jnp.where(lane < head // 2, -1.0, 1.0)

    def put(i, position):
        at = pl.ds(pl.multiple_of(i * block, block), block)
        angle = position.astype(F32) * freq
        cos_ref[at, :] = jnp.cos(angle)
        sin_ref[at, :] = jnp.sin(angle) * sign

    def decode(i, _):
        position = jnp.zeros((block, head), jnp.int32)
        for r in range(block):
            position = jnp.where(sub == r, len_ref[i * block + r], position)
        put(i, position)
        return 0

    def prefill(i, _):
        put(i, sub + (i * block - dec_rows + len_ref[dec_rows]))
        return 0

    lax.fori_loop(0, dec_rows // block, decode, 0)
    lax.fori_loop(dec_rows // block, rows // block, prefill, 0)


def norm_rows(h_ref, gain, b_ref, row0, rows, block=16):
    half = h_ref.shape[2]
    gain_lo, gain_hi = gain[:, :half], gain[:, half:]

    def step(i, _):
        src = pl.ds(pl.multiple_of(row0 + i * block, block), block)
        dst = pl.ds(pl.multiple_of(i * block, block), block)
        lo, hi = h_ref[0, src, :].astype(F32), h_ref[1, src, :].astype(F32)
        total = jnp.sum(lo * lo, axis=-1, keepdims=True) + jnp.sum(hi * hi, axis=-1, keepdims=True)
        inv = lax.rsqrt(total / (2 * half) + EPSILON)
        b_ref[dst, :half] = (lo * inv * gain_lo).astype(BF16)
        b_ref[dst, half:] = (hi * inv * gain_hi).astype(BF16)
        return 0

    lax.fori_loop(0, rows // block, step, 0)


def rope_store(prod, cos, sin, out_ref, rows, col):
    head = cos.shape[1]
    for k in range(prod.shape[1] // head):
        vec = prod[:, k * head:(k + 1) * head].astype(BF16).astype(F32)
        rot = vec * cos + pltpu.roll(vec, head // 2, 1) * sin
        out_ref[rows, pl.ds(col + k * head, head)] = rot.astype(BF16)


def qkv_rows(b_ref, wq_ref, wk_ref, wv_ref, cos_ref, sin_ref, q_ref, k_ref, v_ref, row0, rows):
    rows_at = pl.ds(row0, rows)
    lhs = b_ref[0:rows, :]
    cos, sin = cos_ref[rows_at, :], sin_ref[rows_at, :]

    def q_tile(j, _):
        col = pl.multiple_of(j * TILE, TILE)
        prod = jnp.dot(b_ref[0:rows, :], wq_ref[:, pl.ds(col, TILE)], preferred_element_type=F32)
        rope_store(prod, cos_ref[rows_at, :], sin_ref[rows_at, :], q_ref, rows_at, col)
        return 0

    lax.fori_loop(0, wq_ref.shape[1] // TILE, q_tile, 0)
    rope_store(jnp.dot(lhs, wk_ref[...], preferred_element_type=F32), cos, sin, k_ref, rows_at, 0)
    v_ref[rows_at, :] = jnp.dot(lhs, wv_ref[...], preferred_element_type=F32).astype(BF16)


def qkv_kernel(len_ref, x_hbm, gain_ref, wq_hbm, wk_hbm, wv_hbm, q_ref, k_ref, v_ref, cos_ref, sin_ref, h, b, wq, wk, wv, sems):
    half = h.shape[2]
    copies = [pltpu.make_async_copy(x_hbm.at[:, pl.ds(s * half, half)], h.at[s], sems.at[s]) for s in range(2)]
    copies += [pltpu.make_async_copy(src.at[0], dst, sems.at[2 + n]) for n, (src, dst) in enumerate(((wq_hbm, wq), (wk_hbm, wk), (wv_hbm, wv)))]
    for copy in copies:
        copy.start()
    rope_tables(len_ref, cos_ref, sin_ref)
    copies[0].wait()
    copies[1].wait()
    rows = h.shape[1]
    norm_rows(h, gain_ref[...].astype(F32)[0:1, :], b, 0, rows)
    for copy in copies[2:]:
        copy.wait()
    qkv_rows(b, wq, wk, wv, cos_ref, sin_ref, q_ref, k_ref, v_ref, 0, rows)


def qkv_call(lengths, x, gain, w_q, w_k, w_v, head):
    rows, width = x.shape
    vmem = pl.BlockSpec(memory_space=pltpu.VMEM)
    hbm = pl.BlockSpec(memory_space=pl.ANY)
    return pl.pallas_call(
        qkv_kernel,
        name='qkv_first',
        out_shape=[jax.ShapeDtypeStruct((rows, w.shape[2]), BF16) for w in (w_q, w_k, w_v)] + [jax.ShapeDtypeStruct((rows, head), F32)] * 2,
        in_specs=[pl.BlockSpec(memory_space=pltpu.SMEM), hbm, vmem, hbm, hbm, hbm],
        out_specs=[vmem] * 5,
        scratch_shapes=[
            pltpu.VMEM((2, rows, width // 2), BF16),
            pltpu.VMEM((rows, width), BF16),
            pltpu.VMEM(w_q.shape[1:], BF16),
            pltpu.VMEM(w_k.shape[1:], BF16),
            pltpu.VMEM(w_v.shape[1:], BF16),
            pltpu.SemaphoreType.DMA((5,)),
        ],
        compiler_params=pltpu.CompilerParams(vmem_limit_bytes=61 * 2**20),
    )(lengths, x, gain, w_q, w_k, w_v)


BATCH = 8
SPAN = 256


def length_order(lengths):
    ids = jnp.arange(lengths.shape[0], dtype=jnp.int32)
    lengths = jnp.where(ids == lengths.shape[0] - 1, 0, lengths)
    mine, other = lengths[:, None], lengths[None, :]
    ahead = (other > mine) | ((other == mine) & (ids[None, :] < ids[:, None]))
    rank = jnp.sum(ahead.astype(jnp.int32), axis=1)
    return jnp.sum(jnp.where(rank[None, :] == ids[:, None], ids[None, :], 0), axis=1)


def attention_kernel(layer, len_ref, order_ref, q_hbm, k_hbm, v_hbm, kc_hbm, vc_hbm, o_ref, q_ref, k_ref, v_ref, kbuf, vbuf, qs, kf, vf, sc, od, kp, vp, sems, psems):
    rows = kc_hbm.shape[1] - 1
    seq, head = kc_hbm.shape[3], kc_hbm.shape[4]
    heads = q_ref.shape[1] // head
    kv = kc_hbm.shape[2]
    rep = heads // kv
    scale = head ** -0.5
    steps = rows // BATCH
    spans = seq // SPAN
    nt = (((1,), (1,)), ((), ()))

    def step_spans(step):
        return len_ref[order_ref[step * BATCH]] // SPAN + 1

    def copies(step, slot, n, act):
        at = pl.ds(0, n * SPAN)
        for i in range(BATCH):
            row = order_ref[step * BATCH + i]
            for m, (src, dst) in enumerate(((kc_hbm, kbuf), (vc_hbm, vbuf))):
                copy = pltpu.make_async_copy(src.at[layer, row, :, at, :], dst.at[slot, i, :, at, :], sems.at[slot, i, m])
                if act == 'start':
                    copy.start()
                else:
                    copy.wait()

    def fetch(step, slot):
        for n in range(1, spans + 1):
            @pl.when(step_spans(step) == n)
            def _(n=n):
                copies(step, slot, n, 'start')

    fresh = [pltpu.make_async_copy(src, dst, psems.at[2 + n]) for n, (src, dst) in enumerate(((q_hbm, q_ref), (k_hbm, k_ref), (v_hbm, v_ref)))]
    for copy in fresh:
        copy.start()
    prefill = [pltpu.make_async_copy(src.at[layer, rows], dst, psems.at[n]) for n, (src, dst) in enumerate(((kc_hbm, kp), (vc_hbm, vp)))]
    for copy in prefill:
        copy.start()
    for step in range(SLOTS - 1):
        fetch(step, step)

    qs[...] = jnp.zeros_like(qs)
    for copy in fresh:
        copy.wait()
    for h in range(heads):
        qs[h // rep, pl.ds(h, rows, stride=8), :] = q_ref[0:rows, h * head:(h + 1) * head].astype(F32)
    kf[...] = k_ref[0:rows, :].astype(F32)
    vf[...] = v_ref[0:rows, :].astype(F32)

    for copy in prefill:
        copy.wait()
    limit = len_ref[rows]

    def prefill_head(h, _, keys):
        g = h // rep
        q = q_ref[rows:, pl.ds(pl.multiple_of(h * head, head), head)]
        kn = k_ref[rows:, pl.ds(pl.multiple_of(g * head, head), head)]
        vn = v_ref[rows:, pl.ds(pl.multiple_of(g * head, head), head)]
        s_old = lax.dot_general(q, kp[g, 0:keys, :], nt, preferred_element_type=F32) * scale
        s_new = lax.dot_general(q, kn, nt, preferred_element_type=F32) * scale
        s_old = jnp.where(lax.broadcasted_iota(jnp.int32, s_old.shape, 1) < limit, s_old, -jnp.inf)
        causal = lax.broadcasted_iota(jnp.int32, s_new.shape, 1) <= lax.broadcasted_iota(jnp.int32, s_new.shape, 0)
        s_new = jnp.where(causal, s_new, -jnp.inf)
        top = jnp.maximum(jnp.max(s_old, axis=-1, keepdims=True), jnp.max(s_new, axis=-1, keepdims=True))
        e_old, e_new = jnp.exp(s_old - top), jnp.exp(s_new - top)
        inv = 1.0 / (jnp.sum(e_old, axis=-1, keepdims=True) + jnp.sum(e_new, axis=-1, keepdims=True))
        out = jnp.dot((e_old * inv).astype(BF16), vp[g, 0:keys, :], preferred_element_type=F32)
        out += jnp.dot((e_new * inv).astype(BF16), vn, preferred_element_type=F32)
        o_ref[rows:, pl.ds(pl.multiple_of(h * head, head), head)] = out.astype(BF16)
        return 0

    for n in range(1, spans + 1):
        @pl.when((limit + SPAN - 1) // SPAN == n)
        def _(n=n):
            lax.fori_loop(0, heads, functools.partial(prefill_head, keys=n * SPAN), 0)

    def attend(step, slot, n):
        keys = n * SPAN
        copies(step, slot, n, 'wait')
        for i in range(BATCH):
            row = order_ref[step * BATCH + i]
            length = len_ref[row]
            base = pl.multiple_of((length // 16) * 16, 16)
            hit = lax.broadcasted_iota(jnp.int32, (16, head), 0) == length - base
            near = pl.ds(pl.multiple_of((row // 8) * 8, 8), 8)
            pick = lax.broadcasted_iota(jnp.int32, (8, head), 0) == lax.rem(row, 8)
            for buf, new in ((kbuf, kf), (vbuf, vf)):
                for g in range(kv):
                    old = buf[slot, i, g, pl.ds(base, 16), :].astype(F32)
                    mine = jnp.sum(jnp.where(pick, new[near, g * head:(g + 1) * head], 0.0), axis=0, keepdims=True)
                    buf[slot, i, g, pl.ds(base, 16), :] = jnp.where(hit, mine, old).astype(BF16)
        for i in range(BATCH):
            row = order_ref[step * BATCH + i]
            at = pl.ds(pl.multiple_of(row * 8, 8), 8)
            q = jnp.concatenate([qs[g, at, :] for g in range(kv)], axis=-1).astype(BF16)
            key = jnp.concatenate([kbuf[slot, i, g, 0:keys, :] for g in range(kv)], axis=-1)
            s = lax.dot_general(q, key, nt, preferred_element_type=F32) * scale
            s = jnp.where(lax.broadcasted_iota(jnp.int32, s.shape, 1) <= len_ref[row], s, -jnp.inf)
            sc[i * 8:(i + 1) * 8, 0:keys] = s
        for i in range(BATCH):
            s = sc[i * 8:(i + 1) * 8, 0:keys]
            e = jnp.exp(s - jnp.max(s, axis=-1, keepdims=True))
            p = (e * (1.0 / jnp.sum(e, axis=-1, keepdims=True))).astype(BF16)
            value = jnp.concatenate([vbuf[slot, i, g, 0:keys, :] for g in range(kv)], axis=-1)
            o = jnp.dot(p, value, preferred_element_type=F32)
            own = lax.broadcasted_iota(jnp.int32, (8, head), 0) // rep
            pick = o[:, 0:head]
            for g in range(1, kv):
                pick = jnp.where(own == g, o[:, g * head:(g + 1) * head], pick)
            row = order_ref[step * BATCH + i]
            od[pl.ds(pl.multiple_of(row * 8, 8), 8), :] = pick

    def decode_step(step, _):
        slot = lax.rem(step, SLOTS)

        @pl.when(step + SLOTS - 1 < steps)
        def _():
            fetch(step + SLOTS - 1, lax.rem(step + SLOTS - 1, SLOTS))

        for n in range(1, spans + 1):
            @pl.when(step_spans(step) == n)
            def _(n=n):
                attend(step, slot, n)
        return 0

    lax.fori_loop(0, steps, decode_step, 0)
    for h in range(heads):
        o_ref[0:rows, h * head:(h + 1) * head] = od[pl.ds(h, rows, stride=8), :].astype(BF16)


def attention_call(layer, lengths, order, q, k, v, k_cache, v_cache):
    rows = k_cache.shape[1] - 1
    kv, seq, head = k_cache.shape[2:]
    vmem = pl.BlockSpec(memory_space=pltpu.VMEM)
    hbm = pl.BlockSpec(memory_space=pl.ANY)
    return pl.pallas_call(
        functools.partial(attention_kernel, layer),
        name=f'attention_{layer}',
        out_shape=jax.ShapeDtypeStruct(q.shape, BF16),
        in_specs=[pl.BlockSpec(memory_space=pltpu.SMEM)] * 2 + [hbm] * 5,
        out_specs=vmem,
        scratch_shapes=[
            pltpu.VMEM(q.shape, BF16),
            pltpu.VMEM(k.shape, BF16),
            pltpu.VMEM(v.shape, BF16),
            pltpu.VMEM((SLOTS, BATCH, kv, seq, head), BF16),
            pltpu.VMEM((SLOTS, BATCH, kv, seq, head), BF16),
            pltpu.VMEM((kv, rows * 8, head), F32),
            pltpu.VMEM((rows, kv * head), F32),
            pltpu.VMEM((rows, kv * head), F32),
            pltpu.VMEM((BATCH * 8, seq), F32),
            pltpu.VMEM((rows * 8, head), F32),
            pltpu.VMEM((kv, seq, head), BF16),
            pltpu.VMEM((kv, seq, head), BF16),
            pltpu.SemaphoreType.DMA((SLOTS, BATCH, 2)),
            pltpu.SemaphoreType.DMA((5,)),
        ],
        compiler_params=pltpu.CompilerParams(vmem_limit_bytes=60 * 2**20),
    )(lengths, order, q, k, v, k_cache, v_cache)


def block_kernel(layer, last, groups, *refs):
    if last:
        (x_hbm, att_hbm, gain_ref, wo_hbm, wg_hbm, wu_hbm, wd_hbm, out_ref,
         xh, att, h, part, got, send, cross, b, act, wo, wg, wu, wd, lsem, osem, msem, csem, fsem) = refs
    else:
        (x_hbm, att_hbm, gain_ref, wo_hbm, wg_hbm, wu_hbm, wd_hbm, next_gain_ref, cos_hbm, sin_hbm, wq_hbm, wk_hbm, wv_hbm, out_ref, q_hbm, k_hbm, v_hbm,
         xh, att, h, part, got, send, cross, b, act, wo, wg, wu, wd, wq, wk, wv, cos_ref, sin_ref, q_ref, k_ref, v_ref, lsem, osem, msem, csem, fsem) = refs
    tp = lax.axis_index('tp')
    core = lax.rem(tp, 2)
    mate = tp + 1 - 2 * core
    peer = lax.rem(tp + 2, 4)
    half = h.shape[2]
    own_cols = pl.ds(pl.multiple_of(core * half, half), half)

    loads = [(x_hbm.at[:, own_cols], xh), (att_hbm, att), (wo_hbm.at[layer], wo), (wg_hbm.at[layer], wg), (wu_hbm.at[layer], wu), (wd_hbm.at[layer], wd)]
    if not last:
        loads += [(wq_hbm.at[layer + 1], wq), (wk_hbm.at[layer + 1], wk), (wv_hbm.at[layer + 1], wv), (cos_hbm, cos_ref), (sin_hbm, sin_ref)]
    loads = [pltpu.make_async_copy(src, dst, lsem.at[n]) for n, (src, dst) in enumerate(loads)]
    order = [1, 2, 0] + list(range(3, len(loads)))
    for n in order:
        loads[n].start()

    barrier = pltpu.get_barrier_semaphore()
    for other in (mate, peer):
        pl.semaphore_signal(barrier, inc=1, device_id={'tp': other}, device_id_type=MESH)
    pl.semaphore_wait(barrier, 2)

    def remote(src, dst, sem, idx, device):
        return pltpu.make_async_remote_copy(src_ref=src, dst_ref=dst, send_sem=sem.at[0, idx[0], idx[1]], recv_sem=sem.at[1, idx[0], idx[1]], device_id={'tp': device}, device_id_type=MESH)

    def to_mate(phase, g):
        at = pl.ds(*groups[g])
        return remote(part.at[1 - core, at], got.at[at], msem, (phase, g), mate)

    def to_peer(phase, g):
        at = pl.ds(*groups[g])
        return remote(send.at[at], cross.at[phase, at], csem, (phase, g), peer)

    def final(phase, g):
        at = pl.ds(*groups[g])
        return remote(h.at[core, at], h.at[core, at], fsem, (phase, g), mate)

    def project(lhs_ref, lhs_at, w_ref, g):
        row0, rows = groups[g]
        per_half = half // DOWN_TILE

        def tile(j, _):
            col = pl.multiple_of(j * DOWN_TILE, DOWN_TILE)
            prod = jnp.dot(lhs_ref[lhs_at, :], w_ref[:, pl.ds(col, DOWN_TILE)], preferred_element_type=F32)
            side = j // per_half
            part[side, pl.ds(row0, rows), pl.ds(pl.multiple_of((j - side * per_half) * DOWN_TILE, DOWN_TILE), DOWN_TILE)] = prod.astype(BF16)
            return 0

        lax.fori_loop(0, 2 * per_half, tile, 0, unroll=2)

    def chip_sum(g):
        row0, rows = groups[g]

        def step(i, _):
            at = pl.ds(pl.multiple_of(row0 + i * 16, 16), 16)
            send[at, :] = (part[core, at, :].astype(F32) + got[at, :].astype(F32)).astype(BF16)
            return 0

        lax.fori_loop(0, rows // 16, step, 0)

    def add_sum(phase, g):
        row0, rows = groups[g]

        def step(i, _):
            at = pl.ds(pl.multiple_of(row0 + i * 16, 16), 16)
            base = xh[at, :] if phase == 0 else h[core, at, :]
            total = send[at, :].astype(F32) + cross[phase, at, :].astype(F32)
            h[core, at, :] = (base.astype(F32) + total).astype(BF16)
            return 0

        lax.fori_loop(0, rows // 16, step, 0)

    count = len(groups)

    def arrive(phase, g):
        to_peer(phase, g).wait()
        add_sum(phase, g)
        final(phase, g).start()

    def leave(phase, g):
        to_mate(phase, g).wait()
        chip_sum(g)
        to_peer(phase, g).start()

    loads[1].wait()
    loads[2].wait()
    for g in range(count):
        project(att, pl.ds(*groups[g]), wo, g)
        to_mate(0, g).start()
        if g > 0:
            leave(0, g - 1)
    leave(0, count - 1)
    loads[0].wait()
    mlp_gain = gain_ref[...].astype(F32)[layer:layer + 1, :]
    arrive(0, 0)
    for g in range(count):
        row0, rows = groups[g]
        final(0, g).wait()
        norm_rows(h, mlp_gain, b, row0, rows)
        if g == 0:
            loads[3].wait()
            loads[4].wait()

        def up_tile(j, _, rows=rows):
            cols = pl.ds(pl.multiple_of(j * TILE, TILE), TILE)
            gate = jnp.dot(b[0:rows, :], wg[:, cols], preferred_element_type=F32)
            up = jnp.dot(b[0:rows, :], wu[:, cols], preferred_element_type=F32)
            act[0:rows, cols] = (gate * (1.0 / (1.0 + jnp.exp(-gate))) * up).astype(BF16)
            return 0

        lax.fori_loop(0, wg.shape[1] // TILE, up_tile, 0, unroll=2)
        if g == 0:
            loads[5].wait()
        project(act, pl.ds(0, rows), wd, g)
        to_mate(1, g).start()
        if g + 1 < count:
            arrive(0, g + 1)
        leave(1, g)
    if not last:
        next_gain = next_gain_ref[...].astype(F32)[layer + 1:layer + 2, :]
        for n in range(6, len(loads)):
            loads[n].wait()
    outs = []
    for g in range(len(groups)):
        row0, rows = groups[g]
        arrive(1, g)
        final(1, g).wait()
        at = pl.ds(row0, rows)
        moves = [(h.at[s, at], out_ref.at[at, pl.ds(s * half, half)]) for s in range(2)]
        if not last:
            norm_rows(h, next_gain, b, row0, rows)
            qkv_rows(b, wq, wk, wv, cos_ref, sin_ref, q_ref, k_ref, v_ref, row0, rows)
            moves += [(src.at[at], dst.at[at]) for src, dst in ((q_ref, q_hbm), (k_ref, k_hbm), (v_ref, v_hbm))]
        for n, (src, dst) in enumerate(moves):
            outs.append(pltpu.make_async_copy(src, dst, osem.at[g, n]))
            outs[-1].start()
    for copy in outs:
        copy.wait()


def block_call(layer, last, x, att, mlp_gain, w_o, w_gate, w_up, w_down, extra):
    rows, width = x.shape
    half = width // 2
    most = max(n for _, n in GROUPS)
    count = len(GROUPS)
    vmem = pl.BlockSpec(memory_space=pltpu.VMEM)
    hbm = pl.BlockSpec(memory_space=pl.ANY)
    out_shape = [jax.ShapeDtypeStruct((rows, width), BF16)]
    in_specs = [hbm, hbm, vmem, hbm, hbm, hbm, hbm]
    out_specs = [hbm]
    tables = []
    weights = [w_o, w_gate, w_up, w_down]
    if not last:
        in_specs += [vmem, hbm, hbm, hbm, hbm, hbm]
        weights += list(extra[3:])
        out_shape += [jax.ShapeDtypeStruct((rows, w.shape[2]), BF16) for w in extra[3:]]
        out_specs += [hbm] * 3
        tables = [pltpu.VMEM(extra[1].shape, F32)] * 2 + [pltpu.VMEM((rows, w.shape[2]), BF16) for w in extra[3:]]
    return pl.pallas_call(
        functools.partial(block_kernel, layer, last, GROUPS),
        name=f'block_{layer}',
        out_shape=out_shape,
        in_specs=in_specs,
        out_specs=out_specs,
        scratch_shapes=[
            pltpu.VMEM((rows, half), BF16),
            pltpu.VMEM(att.shape, BF16),
            pltpu.VMEM((2, rows, half), BF16),
            pltpu.VMEM((2, rows, half), BF16),
            pltpu.VMEM((rows, half), BF16),
            pltpu.VMEM((rows, half), BF16),
            pltpu.VMEM((2, rows, half), BF16),
            pltpu.VMEM((most, width), BF16),
            pltpu.VMEM((most, w_down.shape[1]), BF16),
        ] + [pltpu.VMEM(w.shape[1:], BF16) for w in weights] + tables + [
            pltpu.SemaphoreType.DMA((11,)),
            pltpu.SemaphoreType.DMA((count, 5)),
            pltpu.SemaphoreType.DMA((2, 2, count)),
            pltpu.SemaphoreType.DMA((2, 2, count)),
            pltpu.SemaphoreType.DMA((2, 2, count)),
        ],
        compiler_params=pltpu.CompilerParams(collective_id=layer, has_side_effects=True, vmem_limit_bytes=VMEM_LIMIT),
    )(x, att, mlp_gain, w_o, w_gate, w_up, w_down, *extra)


def solution(mesh):
    col_spec = P(None, None, 'tp')
    row_spec = P(None, 'tp', None)
    cache_spec = P(None, 'dp', 'tp', None, None)
    in_specs = (P('dp', None), P('dp'), P(), col_spec, col_spec, col_spec, row_spec, P(), col_spec, col_spec, row_spec, cache_spec, cache_spec)

    def body(x, lengths, attn_gain, w_q, w_k, w_v, w_o, mlp_gain, w_gate, w_up, w_down, k_cache, v_cache):
        layers = w_q.shape[0]
        order = length_order(lengths)
        q, k, v, cos, sin = qkv_call(lengths, x, attn_gain, w_q, w_k, w_v, k_cache.shape[-1])
        for layer in range(layers):
            last = layer == layers - 1
            att = attention_call(layer, lengths, order, q, k, v, k_cache, v_cache)
            extra = () if last else (attn_gain, cos, sin, w_q, w_k, w_v)
            x, *rest = block_call(layer, last, x, att, mlp_gain, w_o, w_gate, w_up, w_down, extra)
            if not last:
                q, k, v = rest
        return x

    return jax.shard_map(body, mesh=mesh, in_specs=in_specs, out_specs=P('dp', None), check_vma=False)
```

```python
import functools
import math

import jax
import jax.numpy as jnp
from jax import lax
from jax.experimental import pallas as pl
from jax.experimental.pallas import tpu as pltpu
from jax.sharding import PartitionSpec as P

ROPE_BASE = 500000.0
EPSILON = 1e-5
MESH = pl.DeviceIdType.MESH
F32 = jnp.float32
BF16 = jnp.bfloat16
VMEM_LIMIT = 64_600_000
TILE = 256
DOWN_TILE = 512
SLOTS = 3
GROUPS = ((0, 112), (112, 112), (224, 96))


def rope_tables(len_ref, cos_ref, sin_ref):
    rows, head = cos_ref.shape
    dec_rows = len_ref.shape[0] - 1
    block = 32
    lane = lax.broadcasted_iota(jnp.int32, (block, head), 1)
    sub = lax.broadcasted_iota(jnp.int32, (block, head), 0)
    freq = jnp.exp(lax.rem(lane, head // 2).astype(F32) * (-2.0 / head * math.log(ROPE_BASE)))
    sign = jnp.where(lane < head // 2, -1.0, 1.0)

    def put(i, position):
        at = pl.ds(pl.multiple_of(i * block, block), block)
        angle = position.astype(F32) * freq
        cos_ref[at, :] = jnp.cos(angle)
        sin_ref[at, :] = jnp.sin(angle) * sign

    def decode(i, _):
        position = jnp.zeros((block, head), jnp.int32)
        for r in range(block):
            position = jnp.where(sub == r, len_ref[i * block + r], position)
        put(i, position)
        return 0

    def prefill(i, _):
        put(i, sub + (i * block - dec_rows + len_ref[dec_rows]))
        return 0

    lax.fori_loop(0, dec_rows // block, decode, 0)
    lax.fori_loop(dec_rows // block, rows // block, prefill, 0)


def norm_rows(h_ref, gain, b_ref, row0, rows, block=16):
    half = h_ref.shape[2]
    gain_lo, gain_hi = gain[:, :half], gain[:, half:]

    def step(i, _):
        src = pl.ds(pl.multiple_of(row0 + i * block, block), block)
        dst = pl.ds(pl.multiple_of(i * block, block), block)
        lo, hi = h_ref[0, src, :].astype(F32), h_ref[1, src, :].astype(F32)
        total = jnp.sum(lo * lo, axis=-1, keepdims=True) + jnp.sum(hi * hi, axis=-1, keepdims=True)
        inv = lax.rsqrt(total / (2 * half) + EPSILON)
        b_ref[dst, :half] = (lo * inv * gain_lo).astype(BF16)
        b_ref[dst, half:] = (hi * inv * gain_hi).astype(BF16)
        return 0

    lax.fori_loop(0, rows // block, step, 0)


def rope_store(prod, cos, sin, out_ref, rows, col):
    head = cos.shape[1]
    for k in range(prod.shape[1] // head):
        vec = prod[:, k * head:(k + 1) * head].astype(BF16).astype(F32)
        rot = vec * cos + pltpu.roll(vec, head // 2, 1) * sin
        out_ref[rows, pl.ds(col + k * head, head)] = rot.astype(BF16)


def qkv_rows(b_ref, wq_ref, wk_ref, wv_ref, cos_ref, sin_ref, q_ref, k_ref, v_ref, row0, rows):
    rows_at = pl.ds(row0, rows)
    lhs = b_ref[0:rows, :]
    cos, sin = cos_ref[rows_at, :], sin_ref[rows_at, :]

    def q_tile(j, _):
        col = pl.multiple_of(j * TILE, TILE)
        prod = jnp.dot(b_ref[0:rows, :], wq_ref[:, pl.ds(col, TILE)], preferred_element_type=F32)
        rope_store(prod, cos_ref[rows_at, :], sin_ref[rows_at, :], q_ref, rows_at, col)
        return 0

    lax.fori_loop(0, wq_ref.shape[1] // TILE, q_tile, 0)
    rope_store(jnp.dot(lhs, wk_ref[...], preferred_element_type=F32), cos, sin, k_ref, rows_at, 0)
    v_ref[rows_at, :] = jnp.dot(lhs, wv_ref[...], preferred_element_type=F32).astype(BF16)


def qkv_kernel(len_ref, x_hbm, gain_ref, wq_hbm, wk_hbm, wv_hbm, q_ref, k_ref, v_ref, cos_ref, sin_ref, h, b, wq, wk, wv, sems):
    half = h.shape[2]
    copies = [pltpu.make_async_copy(x_hbm.at[:, pl.ds(s * half, half)], h.at[s], sems.at[s]) for s in range(2)]
    copies += [pltpu.make_async_copy(src.at[0], dst, sems.at[2 + n]) for n, (src, dst) in enumerate(((wq_hbm, wq), (wk_hbm, wk), (wv_hbm, wv)))]
    for copy in copies:
        copy.start()
    rope_tables(len_ref, cos_ref, sin_ref)
    copies[0].wait()
    copies[1].wait()
    rows = h.shape[1]
    norm_rows(h, gain_ref[...].astype(F32)[0:1, :], b, 0, rows)
    for copy in copies[2:]:
        copy.wait()
    qkv_rows(b, wq, wk, wv, cos_ref, sin_ref, q_ref, k_ref, v_ref, 0, rows)


def qkv_call(lengths, x, gain, w_q, w_k, w_v, head):
    rows, width = x.shape
    vmem = pl.BlockSpec(memory_space=pltpu.VMEM)
    hbm = pl.BlockSpec(memory_space=pl.ANY)
    return pl.pallas_call(
        qkv_kernel,
        name='qkv_first',
        out_shape=[jax.ShapeDtypeStruct((rows, w.shape[2]), BF16) for w in (w_q, w_k, w_v)] + [jax.ShapeDtypeStruct((rows, head), F32)] * 2,
        in_specs=[pl.BlockSpec(memory_space=pltpu.SMEM), hbm, vmem, hbm, hbm, hbm],
        out_specs=[vmem] * 5,
        scratch_shapes=[
            pltpu.VMEM((2, rows, width // 2), BF16),
            pltpu.VMEM((rows, width), BF16),
            pltpu.VMEM(w_q.shape[1:], BF16),
            pltpu.VMEM(w_k.shape[1:], BF16),
            pltpu.VMEM(w_v.shape[1:], BF16),
            pltpu.SemaphoreType.DMA((5,)),
        ],
        compiler_params=pltpu.CompilerParams(vmem_limit_bytes=61 * 2**20),
    )(lengths, x, gain, w_q, w_k, w_v)


BATCH = 8
SPAN = 256


def length_order(lengths):
    ids = jnp.arange(lengths.shape[0], dtype=jnp.int32)
    lengths = jnp.where(ids == lengths.shape[0] - 1, 0, lengths)
    mine, other = lengths[:, None], lengths[None, :]
    ahead = (other > mine) | ((other == mine) & (ids[None, :] < ids[:, None]))
    rank = jnp.sum(ahead.astype(jnp.int32), axis=1)
    return jnp.sum(jnp.where(rank[None, :] == ids[:, None], ids[None, :], 0), axis=1)


def attention_kernel(layer, len_ref, order_ref, q_hbm, k_hbm, v_hbm, kc_hbm, vc_hbm, o_ref, q_ref, k_ref, v_ref, kbuf, vbuf, qs, kf, vf, sc, od, kp, vp, sems, psems):
    rows = kc_hbm.shape[1] - 1
    seq, head = kc_hbm.shape[3], kc_hbm.shape[4]
    heads = q_ref.shape[1] // head
    kv = kc_hbm.shape[2]
    rep = heads // kv
    scale = head ** -0.5
    steps = rows // BATCH
    spans = seq // SPAN
    nt = (((1,), (1,)), ((), ()))

    def step_spans(step):
        return len_ref[order_ref[step * BATCH]] // SPAN + 1

    def copies(step, slot, n, act):
        at = pl.ds(0, n * SPAN)
        for i in range(BATCH):
            row = order_ref[step * BATCH + i]
            for m, (src, dst) in enumerate(((kc_hbm, kbuf), (vc_hbm, vbuf))):
                copy = pltpu.make_async_copy(src.at[layer, row, :, at, :], dst.at[slot, i, :, at, :], sems.at[slot, i, m])
                if act == 'start':
                    copy.start()
                else:
                    copy.wait()

    def fetch(step, slot):
        for n in range(1, spans + 1):
            @pl.when(step_spans(step) == n)
            def _(n=n):
                copies(step, slot, n, 'start')

    fresh = [pltpu.make_async_copy(src, dst, psems.at[2 + n]) for n, (src, dst) in enumerate(((q_hbm, q_ref), (k_hbm, k_ref), (v_hbm, v_ref)))]
    for copy in fresh:
        copy.start()
    prefill = [pltpu.make_async_copy(src.at[layer, rows], dst, psems.at[n]) for n, (src, dst) in enumerate(((kc_hbm, kp), (vc_hbm, vp)))]
    for copy in prefill:
        copy.start()
    qs[...] = jnp.zeros_like(qs)
    for copy in fresh:
        copy.wait()
    fetch(0, 0)
    for h in range(heads):
        qs[h // rep, pl.ds(h, rows, stride=8), :] = q_ref[0:rows, h * head:(h + 1) * head].astype(F32)
    kf[...] = k_ref[0:rows, :].astype(F32)
    vf[...] = v_ref[0:rows, :].astype(F32)

    for copy in prefill:
        copy.wait()
    for step in range(1, SLOTS - 1):
        fetch(step, step)
    limit = len_ref[rows]

    def prefill_head(h, _, keys):
        g = h // rep
        q = q_ref[rows:, pl.ds(pl.multiple_of(h * head, head), head)]
        kn = k_ref[rows:, pl.ds(pl.multiple_of(g * head, head), head)]
        vn = v_ref[rows:, pl.ds(pl.multiple_of(g * head, head), head)]
        s_old = lax.dot_general(q, kp[g, 0:keys, :], nt, preferred_element_type=F32) * scale
        s_new = lax.dot_general(q, kn, nt, preferred_element_type=F32) * scale
        s_old = jnp.where(lax.broadcasted_iota(jnp.int32, s_old.shape, 1) < limit, s_old, -jnp.inf)
        causal = lax.broadcasted_iota(jnp.int32, s_new.shape, 1) <= lax.broadcasted_iota(jnp.int32, s_new.shape, 0)
        s_new = jnp.where(causal, s_new, -jnp.inf)
        top = jnp.maximum(jnp.max(s_old, axis=-1, keepdims=True), jnp.max(s_new, axis=-1, keepdims=True))
        e_old, e_new = jnp.exp(s_old - top), jnp.exp(s_new - top)
        inv = 1.0 / (jnp.sum(e_old, axis=-1, keepdims=True) + jnp.sum(e_new, axis=-1, keepdims=True))
        out = jnp.dot((e_old * inv).astype(BF16), vp[g, 0:keys, :], preferred_element_type=F32)
        out += jnp.dot((e_new * inv).astype(BF16), vn, preferred_element_type=F32)
        o_ref[rows:, pl.ds(pl.multiple_of(h * head, head), head)] = out.astype(BF16)
        return 0

    for n in range(1, spans + 1):
        @pl.when((limit + SPAN - 1) // SPAN == n)
        def _(n=n):
            lax.fori_loop(0, heads, functools.partial(prefill_head, keys=n * SPAN), 0)

    def attend(step, slot, n):
        keys = n * SPAN
        copies(step, slot, n, 'wait')
        for i in range(BATCH):
            row = order_ref[step * BATCH + i]
            length = len_ref[row]
            base = pl.multiple_of((length // 16) * 16, 16)
            hit = lax.broadcasted_iota(jnp.int32, (16, head), 0) == length - base
            near = pl.ds(pl.multiple_of((row // 8) * 8, 8), 8)
            pick = lax.broadcasted_iota(jnp.int32, (8, head), 0) == lax.rem(row, 8)
            for buf, new in ((kbuf, kf), (vbuf, vf)):
                for g in range(kv):
                    old = buf[slot, i, g, pl.ds(base, 16), :].astype(F32)
                    mine = jnp.sum(jnp.where(pick, new[near, g * head:(g + 1) * head], 0.0), axis=0, keepdims=True)
                    buf[slot, i, g, pl.ds(base, 16), :] = jnp.where(hit, mine, old).astype(BF16)
        for i in range(BATCH):
            row = order_ref[step * BATCH + i]
            at = pl.ds(pl.multiple_of(row * 8, 8), 8)
            q = jnp.concatenate([qs[g, at, :] for g in range(kv)], axis=-1).astype(BF16)
            key = jnp.concatenate([kbuf[slot, i, g, 0:keys, :] for g in range(kv)], axis=-1)
            s = lax.dot_general(q, key, nt, preferred_element_type=F32) * scale
            s = jnp.where(lax.broadcasted_iota(jnp.int32, s.shape, 1) <= len_ref[row], s, -jnp.inf)
            sc[i * 8:(i + 1) * 8, 0:keys] = s
        for i in range(BATCH):
            s = sc[i * 8:(i + 1) * 8, 0:keys]
            e = jnp.exp(s - jnp.max(s, axis=-1, keepdims=True))
            p = (e * (1.0 / jnp.sum(e, axis=-1, keepdims=True))).astype(BF16)
            value = jnp.concatenate([vbuf[slot, i, g, 0:keys, :] for g in range(kv)], axis=-1)
            o = jnp.dot(p, value, preferred_element_type=F32)
            own = lax.broadcasted_iota(jnp.int32, (8, head), 0) // rep
            pick = o[:, 0:head]
            for g in range(1, kv):
                pick = jnp.where(own == g, o[:, g * head:(g + 1) * head], pick)
            row = order_ref[step * BATCH + i]
            od[pl.ds(pl.multiple_of(row * 8, 8), 8), :] = pick

    def decode_step(step, _):
        slot = lax.rem(step, SLOTS)

        @pl.when(step + SLOTS - 1 < steps)
        def _():
            fetch(step + SLOTS - 1, lax.rem(step + SLOTS - 1, SLOTS))

        for n in range(1, spans + 1):
            @pl.when(step_spans(step) == n)
            def _(n=n):
                attend(step, slot, n)
        return 0

    lax.fori_loop(0, steps, decode_step, 0)
    for h in range(heads):
        o_ref[0:rows, h * head:(h + 1) * head] = od[pl.ds(h, rows, stride=8), :].astype(BF16)


def attention_call(layer, lengths, order, q, k, v, k_cache, v_cache):
    rows = k_cache.shape[1] - 1
    kv, seq, head = k_cache.shape[2:]
    vmem = pl.BlockSpec(memory_space=pltpu.VMEM)
    hbm = pl.BlockSpec(memory_space=pl.ANY)
    return pl.pallas_call(
        functools.partial(attention_kernel, layer),
        name=f'attention_{layer}',
        out_shape=jax.ShapeDtypeStruct(q.shape, BF16),
        in_specs=[pl.BlockSpec(memory_space=pltpu.SMEM)] * 2 + [hbm] * 5,
        out_specs=vmem,
        scratch_shapes=[
            pltpu.VMEM(q.shape, BF16),
            pltpu.VMEM(k.shape, BF16),
            pltpu.VMEM(v.shape, BF16),
            pltpu.VMEM((SLOTS, BATCH, kv, seq, head), BF16),
            pltpu.VMEM((SLOTS, BATCH, kv, seq, head), BF16),
            pltpu.VMEM((kv, rows * 8, head), F32),
            pltpu.VMEM((rows, kv * head), F32),
            pltpu.VMEM((rows, kv * head), F32),
            pltpu.VMEM((BATCH * 8, seq), F32),
            pltpu.VMEM((rows * 8, head), F32),
            pltpu.VMEM((kv, seq, head), BF16),
            pltpu.VMEM((kv, seq, head), BF16),
            pltpu.SemaphoreType.DMA((SLOTS, BATCH, 2)),
            pltpu.SemaphoreType.DMA((5,)),
        ],
        compiler_params=pltpu.CompilerParams(vmem_limit_bytes=60 * 2**20),
    )(lengths, order, q, k, v, k_cache, v_cache)


def block_kernel(layer, last, groups, *refs):
    if last:
        (x_hbm, att_hbm, gain_ref, wo_hbm, wg_hbm, wu_hbm, wd_hbm, out_ref,
         xh, att, h, part, got, send, cross, b, act, wo, wg, wu, wd, lsem, osem, msem, csem, fsem) = refs
    else:
        (x_hbm, att_hbm, gain_ref, wo_hbm, wg_hbm, wu_hbm, wd_hbm, next_gain_ref, cos_hbm, sin_hbm, wq_hbm, wk_hbm, wv_hbm, out_ref, q_hbm, k_hbm, v_hbm,
         xh, att, h, part, got, send, cross, b, act, wo, wg, wu, wd, wq, wk, wv, cos_ref, sin_ref, q_ref, k_ref, v_ref, lsem, osem, msem, csem, fsem) = refs
    tp = lax.axis_index('tp')
    core = lax.rem(tp, 2)
    mate = tp + 1 - 2 * core
    peer = lax.rem(tp + 2, 4)
    half = h.shape[2]
    own_cols = pl.ds(pl.multiple_of(core * half, half), half)

    loads = [(x_hbm.at[:, own_cols], xh), (att_hbm, att), (wo_hbm.at[layer], wo), (wg_hbm.at[layer], wg), (wu_hbm.at[layer], wu), (wd_hbm.at[layer], wd)]
    if not last:
        loads += [(wq_hbm.at[layer + 1], wq), (wk_hbm.at[layer + 1], wk), (wv_hbm.at[layer + 1], wv), (cos_hbm, cos_ref), (sin_hbm, sin_ref)]
    loads = [pltpu.make_async_copy(src, dst, lsem.at[n]) for n, (src, dst) in enumerate(loads)]
    for n in (1, 2, 0):
        loads[n].start()

    barrier = pltpu.get_barrier_semaphore()
    for other in (mate, peer):
        pl.semaphore_signal(barrier, inc=1, device_id={'tp': other}, device_id_type=MESH)
    pl.semaphore_wait(barrier, 2)

    def remote(src, dst, sem, idx, device):
        return pltpu.make_async_remote_copy(src_ref=src, dst_ref=dst, send_sem=sem.at[0, idx[0], idx[1]], recv_sem=sem.at[1, idx[0], idx[1]], device_id={'tp': device}, device_id_type=MESH)

    def to_mate(phase, g):
        at = pl.ds(*groups[g])
        return remote(part.at[1 - core, at], got.at[at], msem, (phase, g), mate)

    def to_peer(phase, g):
        at = pl.ds(*groups[g])
        return remote(send.at[at], cross.at[phase, at], csem, (phase, g), peer)

    def final(phase, g):
        at = pl.ds(*groups[g])
        return remote(h.at[core, at], h.at[core, at], fsem, (phase, g), mate)

    def project(lhs_ref, lhs_at, w_ref, g):
        row0, rows = groups[g]
        per_half = half // DOWN_TILE

        def tile(j, _):
            col = pl.multiple_of(j * DOWN_TILE, DOWN_TILE)
            prod = jnp.dot(lhs_ref[lhs_at, :], w_ref[:, pl.ds(col, DOWN_TILE)], preferred_element_type=F32)
            side = j // per_half
            part[side, pl.ds(row0, rows), pl.ds(pl.multiple_of((j - side * per_half) * DOWN_TILE, DOWN_TILE), DOWN_TILE)] = prod.astype(BF16)
            return 0

        lax.fori_loop(0, 2 * per_half, tile, 0, unroll=2)

    def chip_sum(g):
        row0, rows = groups[g]

        def step(i, _):
            at = pl.ds(pl.multiple_of(row0 + i * 16, 16), 16)
            send[at, :] = (part[core, at, :].astype(F32) + got[at, :].astype(F32)).astype(BF16)
            return 0

        lax.fori_loop(0, rows // 16, step, 0)

    def add_sum(phase, g):
        row0, rows = groups[g]

        def step(i, _):
            at = pl.ds(pl.multiple_of(row0 + i * 16, 16), 16)
            base = xh[at, :] if phase == 0 else h[core, at, :]
            total = send[at, :].astype(F32) + cross[phase, at, :].astype(F32)
            h[core, at, :] = (base.astype(F32) + total).astype(BF16)
            return 0

        lax.fori_loop(0, rows // 16, step, 0)

    count = len(groups)

    def arrive(phase, g):
        to_peer(phase, g).wait()
        add_sum(phase, g)
        final(phase, g).start()

    def leave(phase, g):
        to_mate(phase, g).wait()
        chip_sum(g)
        to_peer(phase, g).start()

    loads[1].wait()
    loads[2].wait()
    for n in (3, 4, 5):
        loads[n].start()
    for g in range(count):
        project(att, pl.ds(*groups[g]), wo, g)
        to_mate(0, g).start()
        if g > 0:
            leave(0, g - 1)
    leave(0, count - 1)
    loads[0].wait()
    mlp_gain = gain_ref[...].astype(F32)[layer:layer + 1, :]
    arrive(0, 0)
    for g in range(count):
        row0, rows = groups[g]
        final(0, g).wait()
        norm_rows(h, mlp_gain, b, row0, rows)
        if g == 0:
            loads[3].wait()
            loads[4].wait()

        def up_tile(j, _, rows=rows):
            cols = pl.ds(pl.multiple_of(j * TILE, TILE), TILE)
            gate = jnp.dot(b[0:rows, :], wg[:, cols], preferred_element_type=F32)
            up = jnp.dot(b[0:rows, :], wu[:, cols], preferred_element_type=F32)
            act[0:rows, cols] = (gate * (1.0 / (1.0 + jnp.exp(-gate))) * up).astype(BF16)
            return 0

        lax.fori_loop(0, wg.shape[1] // TILE, up_tile, 0, unroll=2)
        if g == 0:
            loads[5].wait()
            for copy in loads[6:]:
                copy.start()
        project(act, pl.ds(0, rows), wd, g)
        to_mate(1, g).start()
        if g + 1 < count:
            arrive(0, g + 1)
        leave(1, g)
    if not last:
        next_gain = next_gain_ref[...].astype(F32)[layer + 1:layer + 2, :]
        for n in range(6, len(loads)):
            loads[n].wait()
    outs = []
    for g in range(len(groups)):
        row0, rows = groups[g]
        arrive(1, g)
        final(1, g).wait()
        at = pl.ds(row0, rows)
        moves = [(h.at[s, at], out_ref.at[at, pl.ds(s * half, half)]) for s in range(2)]
        if not last:
            norm_rows(h, next_gain, b, row0, rows)
            qkv_rows(b, wq, wk, wv, cos_ref, sin_ref, q_ref, k_ref, v_ref, row0, rows)
            moves += [(src.at[at], dst.at[at]) for src, dst in ((q_ref, q_hbm), (k_ref, k_hbm), (v_ref, v_hbm))]
        for n, (src, dst) in enumerate(moves):
            outs.append(pltpu.make_async_copy(src, dst, osem.at[g, n]))
            outs[-1].start()
    for copy in outs:
        copy.wait()


def block_call(layer, last, x, att, mlp_gain, w_o, w_gate, w_up, w_down, extra):
    rows, width = x.shape
    half = width // 2
    most = max(n for _, n in GROUPS)
    count = len(GROUPS)
    vmem = pl.BlockSpec(memory_space=pltpu.VMEM)
    hbm = pl.BlockSpec(memory_space=pl.ANY)
    out_shape = [jax.ShapeDtypeStruct((rows, width), BF16)]
    in_specs = [hbm, hbm, vmem, hbm, hbm, hbm, hbm]
    out_specs = [hbm]
    tables = []
    weights = [w_o, w_gate, w_up, w_down]
    if not last:
        in_specs += [vmem, hbm, hbm, hbm, hbm, hbm]
        weights += list(extra[3:])
        out_shape += [jax.ShapeDtypeStruct((rows, w.shape[2]), BF16) for w in extra[3:]]
        out_specs += [hbm] * 3
        tables = [pltpu.VMEM(extra[1].shape, F32)] * 2 + [pltpu.VMEM((rows, w.shape[2]), BF16) for w in extra[3:]]
    return pl.pallas_call(
        functools.partial(block_kernel, layer, last, GROUPS),
        name=f'block_{layer}',
        out_shape=out_shape,
        in_specs=in_specs,
        out_specs=out_specs,
        scratch_shapes=[
            pltpu.VMEM((rows, half), BF16),
            pltpu.VMEM(att.shape, BF16),
            pltpu.VMEM((2, rows, half), BF16),
            pltpu.VMEM((2, rows, half), BF16),
            pltpu.VMEM((rows, half), BF16),
            pltpu.VMEM((rows, half), BF16),
            pltpu.VMEM((2, rows, half), BF16),
            pltpu.VMEM((most, width), BF16),
            pltpu.VMEM((most, w_down.shape[1]), BF16),
        ] + [pltpu.VMEM(w.shape[1:], BF16) for w in weights] + tables + [
            pltpu.SemaphoreType.DMA((11,)),
            pltpu.SemaphoreType.DMA((count, 5)),
            pltpu.SemaphoreType.DMA((2, 2, count)),
            pltpu.SemaphoreType.DMA((2, 2, count)),
            pltpu.SemaphoreType.DMA((2, 2, count)),
        ],
        compiler_params=pltpu.CompilerParams(collective_id=layer, has_side_effects=True, vmem_limit_bytes=VMEM_LIMIT),
    )(x, att, mlp_gain, w_o, w_gate, w_up, w_down, *extra)


def solution(mesh):
    col_spec = P(None, None, 'tp')
    row_spec = P(None, 'tp', None)
    cache_spec = P(None, 'dp', 'tp', None, None)
    in_specs = (P('dp', None), P('dp'), P(), col_spec, col_spec, col_spec, row_spec, P(), col_spec, col_spec, row_spec, cache_spec, cache_spec)

    def body(x, lengths, attn_gain, w_q, w_k, w_v, w_o, mlp_gain, w_gate, w_up, w_down, k_cache, v_cache):
        layers = w_q.shape[0]
        order = length_order(lengths)
        q, k, v, cos, sin = qkv_call(lengths, x, attn_gain, w_q, w_k, w_v, k_cache.shape[-1])
        for layer in range(layers):
            last = layer == layers - 1
            att = attention_call(layer, lengths, order, q, k, v, k_cache, v_cache)
            extra = () if last else (attn_gain, cos, sin, w_q, w_k, w_v)
            x, *rest = block_call(layer, last, x, att, mlp_gain, w_o, w_gate, w_up, w_down, extra)
            if not last:
                q, k, v = rest
        return x

    return jax.shard_map(body, mesh=mesh, in_specs=in_specs, out_specs=P('dp', None), check_vma=False)
```

```python
import functools
import math

import jax
import jax.numpy as jnp
from jax import lax
from jax.experimental import pallas as pl
from jax.experimental.pallas import tpu as pltpu
from jax.sharding import PartitionSpec as P

ROPE_BASE = 500000.0
EPSILON = 1e-5
MESH = pl.DeviceIdType.MESH
F32 = jnp.float32
BF16 = jnp.bfloat16
VMEM_LIMIT = 64_600_000
TILE = 256
DOWN_TILE = 512
SLOTS = 3
GROUPS = ((0, 128), (128, 96), (224, 96))


def rope_tables(len_ref, cos_ref, sin_ref):
    rows, head = cos_ref.shape
    dec_rows = len_ref.shape[0] - 1
    block = 32
    lane = lax.broadcasted_iota(jnp.int32, (block, head), 1)
    sub = lax.broadcasted_iota(jnp.int32, (block, head), 0)
    freq = jnp.exp(lax.rem(lane, head // 2).astype(F32) * (-2.0 / head * math.log(ROPE_BASE)))
    sign = jnp.where(lane < head // 2, -1.0, 1.0)

    def put(i, position):
        at = pl.ds(pl.multiple_of(i * block, block), block)
        angle = position.astype(F32) * freq
        cos_ref[at, :] = jnp.cos(angle)
        sin_ref[at, :] = jnp.sin(angle) * sign

    def decode(i, _):
        position = jnp.zeros((block, head), jnp.int32)
        for r in range(block):
            position = jnp.where(sub == r, len_ref[i * block + r], position)
        put(i, position)
        return 0

    def prefill(i, _):
        put(i, sub + (i * block - dec_rows + len_ref[dec_rows]))
        return 0

    lax.fori_loop(0, dec_rows // block, decode, 0)
    lax.fori_loop(dec_rows // block, rows // block, prefill, 0)


def length_order(len_ref, order_ref):
    rows = len_ref.shape[0] - 1
    size = order_ref.shape[1]
    sub8 = lax.broadcasted_iota(jnp.int32, (8, size), 0)
    blocks = []
    for i in range(size // 8):
        block = jnp.full((8, size), -1, jnp.int32)
        for r in range(i * 8, min(i * 8 + 8, rows)):
            block = jnp.where(sub8 == r - i * 8, len_ref[r], block)
        blocks.append(block.astype(F32))
    mine = jnp.concatenate(blocks, axis=0)
    other = mine.T
    sub = lax.broadcasted_iota(jnp.int32, (size, size), 0)
    lane = lax.broadcasted_iota(jnp.int32, (size, size), 1)
    ahead = (other > mine) | ((other == mine) & (lane < sub))
    rank = jnp.sum(jnp.where(ahead, 1.0, 0.0), axis=1, keepdims=True)
    order = jnp.sum(jnp.where(rank == lane.astype(F32), sub.astype(F32), 0.0), axis=0, keepdims=True)
    order_ref[...] = order.astype(jnp.int32)


def norm_rows(h_ref, gain, b_ref, row0, rows, block=16):
    half = h_ref.shape[2]
    gain_lo, gain_hi = gain[:, :half], gain[:, half:]

    def step(i, _):
        src = pl.ds(pl.multiple_of(row0 + i * block, block), block)
        dst = pl.ds(pl.multiple_of(i * block, block), block)
        lo, hi = h_ref[0, src, :].astype(F32), h_ref[1, src, :].astype(F32)
        total = jnp.sum(lo * lo, axis=-1, keepdims=True) + jnp.sum(hi * hi, axis=-1, keepdims=True)
        inv = lax.rsqrt(total / (2 * half) + EPSILON)
        b_ref[dst, :half] = (lo * inv * gain_lo).astype(BF16)
        b_ref[dst, half:] = (hi * inv * gain_hi).astype(BF16)
        return 0

    lax.fori_loop(0, rows // block, step, 0, unroll=2)


def rope_store(prod, cos, sin, out_ref, rows, col):
    head = cos.shape[1]
    for k in range(prod.shape[1] // head):
        vec = prod[:, k * head:(k + 1) * head].astype(BF16).astype(F32)
        rot = vec * cos + pltpu.roll(vec, head // 2, 1) * sin
        out_ref[rows, pl.ds(col + k * head, head)] = rot.astype(BF16)


def qkv_rows(b_ref, wq_ref, wk_ref, wv_ref, cos_ref, sin_ref, q_ref, k_ref, v_ref, row0, rows):
    rows_at = pl.ds(row0, rows)
    lhs = b_ref[0:rows, :]
    cos, sin = cos_ref[rows_at, :], sin_ref[rows_at, :]

    def q_tile(j, _):
        col = pl.multiple_of(j * TILE, TILE)
        prod = jnp.dot(b_ref[0:rows, :], wq_ref[:, pl.ds(col, TILE)], preferred_element_type=F32)
        rope_store(prod, cos_ref[rows_at, :], sin_ref[rows_at, :], q_ref, rows_at, col)
        return 0

    lax.fori_loop(0, wq_ref.shape[1] // TILE, q_tile, 0, unroll=True)
    rope_store(jnp.dot(lhs, wk_ref[...], preferred_element_type=F32), cos, sin, k_ref, rows_at, 0)
    v_ref[rows_at, :] = jnp.dot(lhs, wv_ref[...], preferred_element_type=F32).astype(BF16)


def qkv_kernel(len_ref, x_hbm, gain_ref, wq_hbm, wk_hbm, wv_hbm, q_ref, k_ref, v_ref, cos_ref, sin_ref, order_ref, h, b, wq, wk, wv, sems):
    half = h.shape[2]
    copies = [pltpu.make_async_copy(x_hbm.at[:, pl.ds(s * half, half)], h.at[s], sems.at[s]) for s in range(2)]
    copies += [pltpu.make_async_copy(src.at[0], dst, sems.at[2 + n]) for n, (src, dst) in enumerate(((wq_hbm, wq), (wk_hbm, wk), (wv_hbm, wv)))]
    for copy in copies:
        copy.start()
    rope_tables(len_ref, cos_ref, sin_ref)
    length_order(len_ref, order_ref)
    copies[0].wait()
    copies[1].wait()
    rows = h.shape[1]
    norm_rows(h, gain_ref[...].astype(F32)[0:1, :], b, 0, rows)
    for copy in copies[2:]:
        copy.wait()
    qkv_rows(b, wq, wk, wv, cos_ref, sin_ref, q_ref, k_ref, v_ref, 0, rows)


def qkv_call(lengths, x, gain, w_q, w_k, w_v, head):
    rows, width = x.shape
    vmem = pl.BlockSpec(memory_space=pltpu.VMEM)
    hbm = pl.BlockSpec(memory_space=pl.ANY)
    return pl.pallas_call(
        qkv_kernel,
        name='qkv_first',
        out_shape=[jax.ShapeDtypeStruct((rows, w.shape[2]), BF16) for w in (w_q, w_k, w_v)] + [jax.ShapeDtypeStruct((rows, head), F32)] * 2 + [jax.ShapeDtypeStruct((1, 128), jnp.int32)],
        in_specs=[pl.BlockSpec(memory_space=pltpu.SMEM), hbm, vmem, hbm, hbm, hbm],
        out_specs=[vmem] * 6,
        scratch_shapes=[
            pltpu.VMEM((2, rows, width // 2), BF16),
            pltpu.VMEM((rows, width), BF16),
            pltpu.VMEM(w_q.shape[1:], BF16),
            pltpu.VMEM(w_k.shape[1:], BF16),
            pltpu.VMEM(w_v.shape[1:], BF16),
            pltpu.SemaphoreType.DMA((5,)),
        ],
        compiler_params=pltpu.CompilerParams(vmem_limit_bytes=61 * 2**20),
    )(lengths, x, gain, w_q, w_k, w_v)


BATCH = 8
SPAN = 256


def attention_kernel(layer, len_ref, order_ref, q_hbm, k_hbm, v_hbm, kc_hbm, vc_hbm, o_ref, q_ref, k_ref, v_ref, kbuf, vbuf, qs, kf, vf, sc, od, kp, vp, sems, psems):
    rows = kc_hbm.shape[1] - 1
    seq, head = kc_hbm.shape[3], kc_hbm.shape[4]
    heads = q_ref.shape[1] // head
    kv = kc_hbm.shape[2]
    rep = heads // kv
    scale = head ** -0.5
    steps = rows // BATCH
    spans = seq // SPAN
    nt = (((1,), (1,)), ((), ()))

    def step_spans(step):
        return len_ref[order_ref[0, step * BATCH]] // SPAN + 1

    def copies(step, slot, n, act):
        at = pl.ds(0, n * SPAN)
        for i in range(BATCH):
            row = order_ref[0, step * BATCH + i]
            for m, (src, dst) in enumerate(((kc_hbm, kbuf), (vc_hbm, vbuf))):
                copy = pltpu.make_async_copy(src.at[layer, row, :, at, :], dst.at[slot, i, :, at, :], sems.at[slot, i, m])
                if act == 'start':
                    copy.start()
                else:
                    copy.wait()

    def fetch(step, slot):
        for n in range(1, spans + 1):
            @pl.when(step_spans(step) == n)
            def _(n=n):
                copies(step, slot, n, 'start')

    fresh = [pltpu.make_async_copy(src, dst, psems.at[2 + n]) for n, (src, dst) in enumerate(((q_hbm, q_ref), (k_hbm, k_ref), (v_hbm, v_ref)))]
    for copy in fresh:
        copy.start()
    prefill = [pltpu.make_async_copy(src.at[layer, rows], dst, psems.at[n]) for n, (src, dst) in enumerate(((kc_hbm, kp), (vc_hbm, vp)))]
    for copy in prefill:
        copy.start()
    qs[...] = jnp.zeros_like(qs)
    for copy in fresh:
        copy.wait()
    fetch(0, 0)
    for h in range(heads):
        qs[h // rep, pl.ds(h, rows, stride=8), :] = q_ref[0:rows, h * head:(h + 1) * head].astype(F32)
    kf[...] = k_ref[0:rows, :].astype(F32)
    vf[...] = v_ref[0:rows, :].astype(F32)

    for copy in prefill:
        copy.wait()
    for step in range(1, SLOTS - 1):
        fetch(step, step)
    limit = len_ref[rows]

    def prefill_head(h, _, keys):
        g = h // rep
        q = q_ref[rows:, pl.ds(pl.multiple_of(h * head, head), head)]
        kn = k_ref[rows:, pl.ds(pl.multiple_of(g * head, head), head)]
        vn = v_ref[rows:, pl.ds(pl.multiple_of(g * head, head), head)]
        s_old = lax.dot_general(q, kp[g, 0:keys, :], nt, preferred_element_type=F32) * scale
        s_new = lax.dot_general(q, kn, nt, preferred_element_type=F32) * scale
        s_old = jnp.where(lax.broadcasted_iota(jnp.int32, s_old.shape, 1) < limit, s_old, -jnp.inf)
        causal = lax.broadcasted_iota(jnp.int32, s_new.shape, 1) <= lax.broadcasted_iota(jnp.int32, s_new.shape, 0)
        s_new = jnp.where(causal, s_new, -jnp.inf)
        top = jnp.maximum(jnp.max(s_old, axis=-1, keepdims=True), jnp.max(s_new, axis=-1, keepdims=True))
        e_old, e_new = jnp.exp(s_old - top), jnp.exp(s_new - top)
        inv = 1.0 / (jnp.sum(e_old, axis=-1, keepdims=True) + jnp.sum(e_new, axis=-1, keepdims=True))
        out = jnp.dot((e_old * inv).astype(BF16), vp[g, 0:keys, :], preferred_element_type=F32)
        out += jnp.dot((e_new * inv).astype(BF16), vn, preferred_element_type=F32)
        o_ref[rows:, pl.ds(pl.multiple_of(h * head, head), head)] = out.astype(BF16)
        return 0

    for n in range(1, spans + 1):
        @pl.when((limit + SPAN - 1) // SPAN == n)
        def _(n=n):
            lax.fori_loop(0, heads, functools.partial(prefill_head, keys=n * SPAN), 0)

    def attend(step, slot, n):
        keys = n * SPAN
        copies(step, slot, n, 'wait')
        for i in range(BATCH):
            row = order_ref[0, step * BATCH + i]
            length = len_ref[row]
            base = pl.multiple_of((length // 16) * 16, 16)
            hit = lax.broadcasted_iota(jnp.int32, (16, head), 0) == length - base
            near = pl.ds(pl.multiple_of((row // 8) * 8, 8), 8)
            pick = lax.broadcasted_iota(jnp.int32, (8, head), 0) == lax.rem(row, 8)
            for buf, new in ((kbuf, kf), (vbuf, vf)):
                for g in range(kv):
                    old = buf[slot, i, g, pl.ds(base, 16), :].astype(F32)
                    mine = jnp.sum(jnp.where(pick, new[near, g * head:(g + 1) * head], 0.0), axis=0, keepdims=True)
                    buf[slot, i, g, pl.ds(base, 16), :] = jnp.where(hit, mine, old).astype(BF16)
        for i in range(BATCH):
            row = order_ref[0, step * BATCH + i]
            at = pl.ds(pl.multiple_of(row * 8, 8), 8)
            q = jnp.concatenate([qs[g, at, :] for g in range(kv)], axis=-1).astype(BF16)
            key = jnp.concatenate([kbuf[slot, i, g, 0:keys, :] for g in range(kv)], axis=-1)
            s = lax.dot_general(q, key, nt, preferred_element_type=F32) * scale
            s = jnp.where(lax.broadcasted_iota(jnp.int32, s.shape, 1) <= len_ref[row], s, -jnp.inf)
            sc[i * 8:(i + 1) * 8, 0:keys] = s
        for i in range(BATCH):
            s = sc[i * 8:(i + 1) * 8, 0:keys]
            e = jnp.exp(s - jnp.max(s, axis=-1, keepdims=True))
            p = (e * (1.0 / jnp.sum(e, axis=-1, keepdims=True))).astype(BF16)
            value = jnp.concatenate([vbuf[slot, i, g, 0:keys, :] for g in range(kv)], axis=-1)
            o = jnp.dot(p, value, preferred_element_type=F32)
            own = lax.broadcasted_iota(jnp.int32, (8, head), 0) // rep
            pick = o[:, 0:head]
            for g in range(1, kv):
                pick = jnp.where(own == g, o[:, g * head:(g + 1) * head], pick)
            row = order_ref[0, step * BATCH + i]
            od[pl.ds(pl.multiple_of(row * 8, 8), 8), :] = pick

    def decode_step(step, _):
        slot = lax.rem(step, SLOTS)

        @pl.when(step + SLOTS - 1 < steps)
        def _():
            fetch(step + SLOTS - 1, lax.rem(step + SLOTS - 1, SLOTS))

        for n in range(1, spans + 1):
            @pl.when(step_spans(step) == n)
            def _(n=n):
                attend(step, slot, n)
        return 0

    lax.fori_loop(0, steps, decode_step, 0)
    for h in range(heads):
        o_ref[0:rows, h * head:(h + 1) * head] = od[pl.ds(h, rows, stride=8), :].astype(BF16)


def attention_call(layer, lengths, order, q, k, v, k_cache, v_cache):
    rows = k_cache.shape[1] - 1
    kv, seq, head = k_cache.shape[2:]
    vmem = pl.BlockSpec(memory_space=pltpu.VMEM)
    hbm = pl.BlockSpec(memory_space=pl.ANY)
    return pl.pallas_call(
        functools.partial(attention_kernel, layer),
        name=f'attention_{layer}',
        out_shape=jax.ShapeDtypeStruct(q.shape, BF16),
        in_specs=[pl.BlockSpec(memory_space=pltpu.SMEM)] * 2 + [hbm] * 5,
        out_specs=vmem,
        scratch_shapes=[
            pltpu.VMEM(q.shape, BF16),
            pltpu.VMEM(k.shape, BF16),
            pltpu.VMEM(v.shape, BF16),
            pltpu.VMEM((SLOTS, BATCH, kv, seq, head), BF16),
            pltpu.VMEM((SLOTS, BATCH, kv, seq, head), BF16),
            pltpu.VMEM((kv, rows * 8, head), F32),
            pltpu.VMEM((rows, kv * head), F32),
            pltpu.VMEM((rows, kv * head), F32),
            pltpu.VMEM((BATCH * 8, seq), F32),
            pltpu.VMEM((rows * 8, head), F32),
            pltpu.VMEM((kv, seq, head), BF16),
            pltpu.VMEM((kv, seq, head), BF16),
            pltpu.SemaphoreType.DMA((SLOTS, BATCH, 2)),
            pltpu.SemaphoreType.DMA((5,)),
        ],
        compiler_params=pltpu.CompilerParams(vmem_limit_bytes=60 * 2**20),
    )(lengths, order, q, k, v, k_cache, v_cache)


def block_kernel(layer, last, groups, *refs):
    if last:
        (x_hbm, att_hbm, gain_ref, wo_hbm, wg_hbm, wu_hbm, wd_hbm, out_ref,
         xh, att, h, part, got, send, cross, b, act, wo, wg, wu, wd, lsem, osem, msem, csem, fsem) = refs
    else:
        (x_hbm, att_hbm, gain_ref, wo_hbm, wg_hbm, wu_hbm, wd_hbm, next_gain_ref, cos_hbm, sin_hbm, wq_hbm, wk_hbm, wv_hbm, out_ref, q_hbm, k_hbm, v_hbm,
         xh, att, h, part, got, send, cross, b, act, wo, wg, wu, wd, wq, wk, wv, cos_ref, sin_ref, q_ref, k_ref, v_ref, lsem, osem, msem, csem, fsem) = refs
    tp = lax.axis_index('tp')
    core = lax.rem(tp, 2)
    mate = tp + 1 - 2 * core
    peer = lax.rem(tp + 2, 4)
    half = h.shape[2]
    own_cols = pl.ds(pl.multiple_of(core * half, half), half)

    loads = [(x_hbm.at[:, own_cols], xh), (att_hbm, att), (wo_hbm.at[layer], wo), (wg_hbm.at[layer], wg), (wu_hbm.at[layer], wu), (wd_hbm.at[layer], wd)]
    if not last:
        loads += [(wq_hbm.at[layer + 1], wq), (wk_hbm.at[layer + 1], wk), (wv_hbm.at[layer + 1], wv), (cos_hbm, cos_ref), (sin_hbm, sin_ref)]
    loads = [pltpu.make_async_copy(src, dst, lsem.at[n]) for n, (src, dst) in enumerate(loads)]
    for n in (1, 2, 0):
        loads[n].start()

    barrier = pltpu.get_barrier_semaphore()
    for other in (mate, peer):
        pl.semaphore_signal(barrier, inc=1, device_id={'tp': other}, device_id_type=MESH)
    pl.semaphore_wait(barrier, 2)

    def remote(src, dst, sem, idx, device):
        return pltpu.make_async_remote_copy(src_ref=src, dst_ref=dst, send_sem=sem.at[0, idx[0], idx[1]], recv_sem=sem.at[1, idx[0], idx[1]], device_id={'tp': device}, device_id_type=MESH)

    def to_mate(phase, g):
        at = pl.ds(*groups[g])
        return remote(part.at[1 - core, at], got.at[at], msem, (phase, g), mate)

    def to_peer(phase, g):
        at = pl.ds(*groups[g])
        return remote(send.at[at], cross.at[phase, at], csem, (phase, g), peer)

    def final(phase, g):
        at = pl.ds(*groups[g])
        return remote(h.at[core, at], h.at[core, at], fsem, (phase, g), mate)

    def project(lhs_ref, lhs_at, w_ref, g):
        row0, rows = groups[g]
        per_half = half // DOWN_TILE

        def tile(j, _):
            col = pl.multiple_of(j * DOWN_TILE, DOWN_TILE)
            prod = jnp.dot(lhs_ref[lhs_at, :], w_ref[:, pl.ds(col, DOWN_TILE)], preferred_element_type=F32)
            side = j // per_half
            part[side, pl.ds(row0, rows), pl.ds(pl.multiple_of((j - side * per_half) * DOWN_TILE, DOWN_TILE), DOWN_TILE)] = prod.astype(BF16)
            return 0

        lax.fori_loop(0, 2 * per_half, tile, 0, unroll=2)

    def chip_sum(g):
        row0, rows = groups[g]

        def step(i, _):
            at = pl.ds(pl.multiple_of(row0 + i * 16, 16), 16)
            send[at, :] = (part[core, at, :].astype(F32) + got[at, :].astype(F32)).astype(BF16)
            return 0

        lax.fori_loop(0, rows // 16, step, 0, unroll=2)

    def add_sum(phase, g):
        row0, rows = groups[g]

        def step(i, _):
            at = pl.ds(pl.multiple_of(row0 + i * 16, 16), 16)
            base = xh[at, :] if phase == 0 else h[core, at, :]
            total = send[at, :].astype(F32) + cross[phase, at, :].astype(F32)
            h[core, at, :] = (base.astype(F32) + total).astype(BF16)
            return 0

        lax.fori_loop(0, rows // 16, step, 0, unroll=2)

    count = len(groups)

    def arrive(phase, g):
        to_peer(phase, g).wait()
        add_sum(phase, g)
        final(phase, g).start()

    def leave(phase, g):
        to_mate(phase, g).wait()
        chip_sum(g)
        to_peer(phase, g).start()

    loads[1].wait()
    loads[2].wait()
    for n in (3, 4, 5):
        loads[n].start()
    for g in range(count):
        project(att, pl.ds(*groups[g]), wo, g)
        to_mate(0, g).start()
        if g > 0:
            leave(0, g - 1)
    leave(0, count - 1)
    loads[0].wait()
    mlp_gain = gain_ref[...].astype(F32)[layer:layer + 1, :]
    arrive(0, 0)
    for g in range(count):
        row0, rows = groups[g]
        final(0, g).wait()
        norm_rows(h, mlp_gain, b, row0, rows)
        if g == 0:
            loads[3].wait()
            loads[4].wait()

        def up_tile(j, _, rows=rows):
            cols = pl.ds(pl.multiple_of(j * TILE, TILE), TILE)
            gate = jnp.dot(b[0:rows, :], wg[:, cols], preferred_element_type=F32)
            up = jnp.dot(b[0:rows, :], wu[:, cols], preferred_element_type=F32)
            act[0:rows, cols] = (gate * (1.0 / (1.0 + jnp.exp(-gate))) * up).astype(BF16)
            return 0

        lax.fori_loop(0, wg.shape[1] // TILE, up_tile, 0, unroll=2)
        if g == 0:
            loads[5].wait()
            for copy in loads[6:]:
                copy.start()
        project(act, pl.ds(0, rows), wd, g)
        to_mate(1, g).start()
        if g + 1 < count:
            arrive(0, g + 1)
        leave(1, g)
    if not last:
        next_gain = next_gain_ref[...].astype(F32)[layer + 1:layer + 2, :]
        for n in range(6, len(loads)):
            loads[n].wait()
    outs = []
    for g in range(len(groups)):
        row0, rows = groups[g]
        arrive(1, g)
        final(1, g).wait()
        at = pl.ds(row0, rows)
        moves = [(h.at[s, at], out_ref.at[at, pl.ds(s * half, half)]) for s in range(2)]
        if not last:
            norm_rows(h, next_gain, b, row0, rows)
            qkv_rows(b, wq, wk, wv, cos_ref, sin_ref, q_ref, k_ref, v_ref, row0, rows)
            moves += [(src.at[at], dst.at[at]) for src, dst in ((q_ref, q_hbm), (k_ref, k_hbm), (v_ref, v_hbm))]
        for n, (src, dst) in enumerate(moves):
            outs.append(pltpu.make_async_copy(src, dst, osem.at[g, n]))
            outs[-1].start()
    for copy in outs:
        copy.wait()


def block_call(layer, last, x, att, mlp_gain, w_o, w_gate, w_up, w_down, extra):
    rows, width = x.shape
    half = width // 2
    most = max(n for _, n in GROUPS)
    count = len(GROUPS)
    vmem = pl.BlockSpec(memory_space=pltpu.VMEM)
    hbm = pl.BlockSpec(memory_space=pl.ANY)
    out_shape = [jax.ShapeDtypeStruct((rows, width), BF16)]
    in_specs = [hbm, hbm, vmem, hbm, hbm, hbm, hbm]
    out_specs = [hbm]
    tables = []
    weights = [w_o, w_gate, w_up, w_down]
    if not last:
        in_specs += [vmem, hbm, hbm, hbm, hbm, hbm]
        weights += list(extra[3:])
        out_shape += [jax.ShapeDtypeStruct((rows, w.shape[2]), BF16) for w in extra[3:]]
        out_specs += [hbm] * 3
        tables = [pltpu.VMEM(extra[1].shape, F32)] * 2 + [pltpu.VMEM((rows, w.shape[2]), BF16) for w in extra[3:]]
    return pl.pallas_call(
        functools.partial(block_kernel, layer, last, GROUPS),
        name=f'block_{layer}',
        out_shape=out_shape,
        in_specs=in_specs,
        out_specs=out_specs,
        scratch_shapes=[
            pltpu.VMEM((rows, half), BF16),
            pltpu.VMEM(att.shape, BF16),
            pltpu.VMEM((2, rows, half), BF16),
            pltpu.VMEM((2, rows, half), BF16),
            pltpu.VMEM((rows, half), BF16),
            pltpu.VMEM((rows, half), BF16),
            pltpu.VMEM((2, rows, half), BF16),
            pltpu.VMEM((most, width), BF16),
            pltpu.VMEM((most, w_down.shape[1]), BF16),
        ] + [pltpu.VMEM(w.shape[1:], BF16) for w in weights] + tables + [
            pltpu.SemaphoreType.DMA((11,)),
            pltpu.SemaphoreType.DMA((count, 5)),
            pltpu.SemaphoreType.DMA((2, 2, count)),
            pltpu.SemaphoreType.DMA((2, 2, count)),
            pltpu.SemaphoreType.DMA((2, 2, count)),
        ],
        compiler_params=pltpu.CompilerParams(collective_id=layer, has_side_effects=True, vmem_limit_bytes=VMEM_LIMIT),
    )(x, att, mlp_gain, w_o, w_gate, w_up, w_down, *extra)


def solution(mesh):
    col_spec = P(None, None, 'tp')
    row_spec = P(None, 'tp', None)
    cache_spec = P(None, 'dp', 'tp', None, None)
    in_specs = (P('dp', None), P('dp'), P(), col_spec, col_spec, col_spec, row_spec, P(), col_spec, col_spec, row_spec, cache_spec, cache_spec)

    def body(x, lengths, attn_gain, w_q, w_k, w_v, w_o, mlp_gain, w_gate, w_up, w_down, k_cache, v_cache):
        layers = w_q.shape[0]
        q, k, v, cos, sin, order = qkv_call(lengths, x, attn_gain, w_q, w_k, w_v, k_cache.shape[-1])
        for layer in range(layers):
            last = layer == layers - 1
            att = attention_call(layer, lengths, order, q, k, v, k_cache, v_cache)
            extra = () if last else (attn_gain, cos, sin, w_q, w_k, w_v)
            x, *rest = block_call(layer, last, x, att, mlp_gain, w_o, w_gate, w_up, w_down, extra)
            if not last:
                q, k, v = rest
        return x

    return jax.shard_map(body, mesh=mesh, in_specs=in_specs, out_specs=P('dp', None), check_vma=False)
```

```python
import functools
import math

import jax
import jax.numpy as jnp
from jax import lax
from jax.experimental import pallas as pl
from jax.experimental.pallas import tpu as pltpu
from jax.sharding import PartitionSpec as P

ROPE_BASE = 500000.0
EPSILON = 1e-5
MESH = pl.DeviceIdType.MESH
F32 = jnp.float32
BF16 = jnp.bfloat16
VMEM_LIMIT = 64_600_000
TILE = 256
DOWN_TILE = 512
SLOTS = 3
GROUPS = ((0, 64), (64, 128), (192, 128))


def rope_tables(len_ref, cos_ref, sin_ref):
    rows, head = cos_ref.shape
    dec_rows = len_ref.shape[0] - 1
    block = 32
    lane = lax.broadcasted_iota(jnp.int32, (block, head), 1)
    sub = lax.broadcasted_iota(jnp.int32, (block, head), 0)
    freq = jnp.exp(lax.rem(lane, head // 2).astype(F32) * (-2.0 / head * math.log(ROPE_BASE)))
    sign = jnp.where(lane < head // 2, -1.0, 1.0)

    def put(i, position):
        at = pl.ds(pl.multiple_of(i * block, block), block)
        angle = position.astype(F32) * freq
        cos_ref[at, :] = jnp.cos(angle)
        sin_ref[at, :] = jnp.sin(angle) * sign

    def decode(i, _):
        position = jnp.zeros((block, head), jnp.int32)
        for r in range(block):
            position = jnp.where(sub == r, len_ref[i * block + r], position)
        put(i, position)
        return 0

    def prefill(i, _):
        put(i, sub + (i * block - dec_rows + len_ref[dec_rows]))
        return 0

    lax.fori_loop(0, dec_rows // block, decode, 0)
    lax.fori_loop(dec_rows // block, rows // block, prefill, 0)


def length_order(len_ref, order_ref):
    rows = len_ref.shape[0] - 1
    size = order_ref.shape[1]
    sub8 = lax.broadcasted_iota(jnp.int32, (8, size), 0)
    blocks = []
    for i in range(size // 8):
        block = jnp.full((8, size), -1, jnp.int32)
        for r in range(i * 8, min(i * 8 + 8, rows)):
            block = jnp.where(sub8 == r - i * 8, len_ref[r], block)
        blocks.append(block.astype(F32))
    mine = jnp.concatenate(blocks, axis=0)
    other = mine.T
    sub = lax.broadcasted_iota(jnp.int32, (size, size), 0)
    lane = lax.broadcasted_iota(jnp.int32, (size, size), 1)
    ahead = (other > mine) | ((other == mine) & (lane < sub))
    rank = jnp.sum(jnp.where(ahead, 1.0, 0.0), axis=1, keepdims=True)
    order = jnp.sum(jnp.where(rank == lane.astype(F32), sub.astype(F32), 0.0), axis=0, keepdims=True)
    order_ref[...] = order.astype(jnp.int32)


def norm_rows(h_ref, gain, b_ref, row0, rows, block=16):
    half = h_ref.shape[2]
    gain_lo, gain_hi = gain[:, :half], gain[:, half:]

    def step(i, _):
        src = pl.ds(pl.multiple_of(row0 + i * block, block), block)
        dst = pl.ds(pl.multiple_of(i * block, block), block)
        lo, hi = h_ref[0, src, :].astype(F32), h_ref[1, src, :].astype(F32)
        total = jnp.sum(lo * lo, axis=-1, keepdims=True) + jnp.sum(hi * hi, axis=-1, keepdims=True)
        inv = lax.rsqrt(total / (2 * half) + EPSILON)
        b_ref[dst, :half] = (lo * inv * gain_lo).astype(BF16)
        b_ref[dst, half:] = (hi * inv * gain_hi).astype(BF16)
        return 0

    lax.fori_loop(0, rows // block, step, 0, unroll=2)


def rope_store(prod, cos, sin, out_ref, rows, col):
    head = cos.shape[1]
    for k in range(prod.shape[1] // head):
        vec = prod[:, k * head:(k + 1) * head].astype(BF16).astype(F32)
        rot = vec * cos + pltpu.roll(vec, head // 2, 1) * sin
        out_ref[rows, pl.ds(col + k * head, head)] = rot.astype(BF16)


def qkv_rows(b_ref, wq_ref, wk_ref, wv_ref, cos_ref, sin_ref, q_ref, k_ref, v_ref, row0, rows):
    rows_at = pl.ds(row0, rows)
    lhs = b_ref[0:rows, :]
    cos, sin = cos_ref[rows_at, :], sin_ref[rows_at, :]

    def q_tile(j, _):
        col = pl.multiple_of(j * TILE, TILE)
        prod = jnp.dot(b_ref[0:rows, :], wq_ref[:, pl.ds(col, TILE)], preferred_element_type=F32)
        rope_store(prod, cos_ref[rows_at, :], sin_ref[rows_at, :], q_ref, rows_at, col)
        return 0

    lax.fori_loop(0, wq_ref.shape[1] // TILE, q_tile, 0, unroll=True)
    rope_store(jnp.dot(lhs, wk_ref[...], preferred_element_type=F32), cos, sin, k_ref, rows_at, 0)
    v_ref[rows_at, :] = jnp.dot(lhs, wv_ref[...], preferred_element_type=F32).astype(BF16)


def qkv_kernel(len_ref, x_hbm, gain_ref, wq_hbm, wk_hbm, wv_hbm, q_ref, k_ref, v_ref, cos_ref, sin_ref, order_ref, h, b, wq, wk, wv, sems):
    half = h.shape[2]
    copies = [pltpu.make_async_copy(x_hbm.at[:, pl.ds(s * half, half)], h.at[s], sems.at[s]) for s in range(2)]
    copies += [pltpu.make_async_copy(src.at[0], dst, sems.at[2 + n]) for n, (src, dst) in enumerate(((wq_hbm, wq), (wk_hbm, wk), (wv_hbm, wv)))]
    for copy in copies:
        copy.start()
    rope_tables(len_ref, cos_ref, sin_ref)
    length_order(len_ref, order_ref)
    copies[0].wait()
    copies[1].wait()
    rows = h.shape[1]
    norm_rows(h, gain_ref[...].astype(F32)[0:1, :], b, 0, rows)
    for copy in copies[2:]:
        copy.wait()
    qkv_rows(b, wq, wk, wv, cos_ref, sin_ref, q_ref, k_ref, v_ref, 0, rows)


def qkv_call(lengths, x, gain, w_q, w_k, w_v, head):
    rows, width = x.shape
    vmem = pl.BlockSpec(memory_space=pltpu.VMEM)
    hbm = pl.BlockSpec(memory_space=pl.ANY)
    return pl.pallas_call(
        qkv_kernel,
        name='qkv_first',
        out_shape=[jax.ShapeDtypeStruct((rows, w.shape[2]), BF16) for w in (w_q, w_k, w_v)] + [jax.ShapeDtypeStruct((rows, head), F32)] * 2 + [jax.ShapeDtypeStruct((1, 128), jnp.int32)],
        in_specs=[pl.BlockSpec(memory_space=pltpu.SMEM), hbm, vmem, hbm, hbm, hbm],
        out_specs=[vmem] * 6,
        scratch_shapes=[
            pltpu.VMEM((2, rows, width // 2), BF16),
            pltpu.VMEM((rows, width), BF16),
            pltpu.VMEM(w_q.shape[1:], BF16),
            pltpu.VMEM(w_k.shape[1:], BF16),
            pltpu.VMEM(w_v.shape[1:], BF16),
            pltpu.SemaphoreType.DMA((5,)),
        ],
        compiler_params=pltpu.CompilerParams(vmem_limit_bytes=61 * 2**20),
    )(lengths, x, gain, w_q, w_k, w_v)


BATCH = 8
SPAN = 256


def attention_kernel(layer, len_ref, order_ref, q_hbm, k_hbm, v_hbm, kc_hbm, vc_hbm, o_ref, q_ref, k_ref, v_ref, kbuf, vbuf, qs, kf, vf, sc, od, kp, vp, sems, psems):
    rows = kc_hbm.shape[1] - 1
    seq, head = kc_hbm.shape[3], kc_hbm.shape[4]
    heads = q_ref.shape[1] // head
    kv = kc_hbm.shape[2]
    rep = heads // kv
    scale = head ** -0.5
    steps = rows // BATCH
    spans = seq // SPAN
    nt = (((1,), (1,)), ((), ()))

    def step_spans(step):
        return len_ref[order_ref[0, step * BATCH]] // SPAN + 1

    def copies(step, slot, n, act):
        at = pl.ds(0, n * SPAN)
        for i in range(BATCH):
            row = order_ref[0, step * BATCH + i]
            for m, (src, dst) in enumerate(((kc_hbm, kbuf), (vc_hbm, vbuf))):
                copy = pltpu.make_async_copy(src.at[layer, row, :, at, :], dst.at[slot, i, :, at, :], sems.at[slot, i, m])
                if act == 'start':
                    copy.start()
                else:
                    copy.wait()

    def fetch(step, slot):
        for n in range(1, spans + 1):
            @pl.when(step_spans(step) == n)
            def _(n=n):
                copies(step, slot, n, 'start')

    fresh = [pltpu.make_async_copy(src, dst, psems.at[2 + n]) for n, (src, dst) in enumerate(((q_hbm, q_ref), (k_hbm, k_ref), (v_hbm, v_ref)))]
    for copy in fresh:
        copy.start()
    prefill = [pltpu.make_async_copy(src.at[layer, rows], dst, psems.at[n]) for n, (src, dst) in enumerate(((kc_hbm, kp), (vc_hbm, vp)))]
    for copy in prefill:
        copy.start()
    qs[...] = jnp.zeros_like(qs)
    for copy in fresh:
        copy.wait()
    fetch(0, 0)
    for h in range(heads):
        qs[h // rep, pl.ds(h, rows, stride=8), :] = q_ref[0:rows, h * head:(h + 1) * head].astype(F32)
    kf[...] = k_ref[0:rows, :].astype(F32)
    vf[...] = v_ref[0:rows, :].astype(F32)

    for copy in prefill:
        copy.wait()
    for step in range(1, SLOTS - 1):
        fetch(step, step)
    limit = len_ref[rows]

    def prefill_head(h, _, keys):
        g = h // rep
        q = q_ref[rows:, pl.ds(pl.multiple_of(h * head, head), head)]
        kn = k_ref[rows:, pl.ds(pl.multiple_of(g * head, head), head)]
        vn = v_ref[rows:, pl.ds(pl.multiple_of(g * head, head), head)]
        s_old = lax.dot_general(q, kp[g, 0:keys, :], nt, preferred_element_type=F32) * scale
        s_new = lax.dot_general(q, kn, nt, preferred_element_type=F32) * scale
        s_old = jnp.where(lax.broadcasted_iota(jnp.int32, s_old.shape, 1) < limit, s_old, -jnp.inf)
        causal = lax.broadcasted_iota(jnp.int32, s_new.shape, 1) <= lax.broadcasted_iota(jnp.int32, s_new.shape, 0)
        s_new = jnp.where(causal, s_new, -jnp.inf)
        top = jnp.maximum(jnp.max(s_old, axis=-1, keepdims=True), jnp.max(s_new, axis=-1, keepdims=True))
        e_old, e_new = jnp.exp(s_old - top), jnp.exp(s_new - top)
        inv = 1.0 / (jnp.sum(e_old, axis=-1, keepdims=True) + jnp.sum(e_new, axis=-1, keepdims=True))
        out = jnp.dot((e_old * inv).astype(BF16), vp[g, 0:keys, :], preferred_element_type=F32)
        out += jnp.dot((e_new * inv).astype(BF16), vn, preferred_element_type=F32)
        o_ref[rows:, pl.ds(pl.multiple_of(h * head, head), head)] = out.astype(BF16)
        return 0

    for n in range(1, spans + 1):
        @pl.when((limit + SPAN - 1) // SPAN == n)
        def _(n=n):
            lax.fori_loop(0, heads, functools.partial(prefill_head, keys=n * SPAN), 0)

    def attend(step, slot, n):
        keys = n * SPAN
        copies(step, slot, n, 'wait')
        for i in range(BATCH):
            row = order_ref[0, step * BATCH + i]
            length = len_ref[row]
            base = pl.multiple_of((length // 16) * 16, 16)
            hit = lax.broadcasted_iota(jnp.int32, (16, head), 0) == length - base
            near = pl.ds(pl.multiple_of((row // 8) * 8, 8), 8)
            pick = lax.broadcasted_iota(jnp.int32, (8, head), 0) == lax.rem(row, 8)
            for buf, new in ((kbuf, kf), (vbuf, vf)):
                for g in range(kv):
                    old = buf[slot, i, g, pl.ds(base, 16), :].astype(F32)
                    mine = jnp.sum(jnp.where(pick, new[near, g * head:(g + 1) * head], 0.0), axis=0, keepdims=True)
                    buf[slot, i, g, pl.ds(base, 16), :] = jnp.where(hit, mine, old).astype(BF16)
        for i in range(BATCH):
            row = order_ref[0, step * BATCH + i]
            at = pl.ds(pl.multiple_of(row * 8, 8), 8)
            q = jnp.concatenate([qs[g, at, :] for g in range(kv)], axis=-1).astype(BF16)
            key = jnp.concatenate([kbuf[slot, i, g, 0:keys, :] for g in range(kv)], axis=-1)
            s = lax.dot_general(q, key, nt, preferred_element_type=F32) * scale
            s = jnp.where(lax.broadcasted_iota(jnp.int32, s.shape, 1) <= len_ref[row], s, -jnp.inf)
            sc[i * 8:(i + 1) * 8, 0:keys] = s
        for i in range(BATCH):
            s = sc[i * 8:(i + 1) * 8, 0:keys]
            e = jnp.exp(s - jnp.max(s, axis=-1, keepdims=True))
            p = (e * (1.0 / jnp.sum(e, axis=-1, keepdims=True))).astype(BF16)
            value = jnp.concatenate([vbuf[slot, i, g, 0:keys, :] for g in range(kv)], axis=-1)
            o = jnp.dot(p, value, preferred_element_type=F32)
            own = lax.broadcasted_iota(jnp.int32, (8, head), 0) // rep
            pick = o[:, 0:head]
            for g in range(1, kv):
                pick = jnp.where(own == g, o[:, g * head:(g + 1) * head], pick)
            row = order_ref[0, step * BATCH + i]
            od[pl.ds(pl.multiple_of(row * 8, 8), 8), :] = pick

    def decode_step(step, _):
        slot = lax.rem(step, SLOTS)

        @pl.when(step + SLOTS - 1 < steps)
        def _():
            fetch(step + SLOTS - 1, lax.rem(step + SLOTS - 1, SLOTS))

        for n in range(1, spans + 1):
            @pl.when(step_spans(step) == n)
            def _(n=n):
                attend(step, slot, n)
        return 0

    lax.fori_loop(0, steps, decode_step, 0)
    for h in range(heads):
        o_ref[0:rows, h * head:(h + 1) * head] = od[pl.ds(h, rows, stride=8), :].astype(BF16)


def attention_call(layer, lengths, order, q, k, v, k_cache, v_cache):
    rows = k_cache.shape[1] - 1
    kv, seq, head = k_cache.shape[2:]
    vmem = pl.BlockSpec(memory_space=pltpu.VMEM)
    hbm = pl.BlockSpec(memory_space=pl.ANY)
    return pl.pallas_call(
        functools.partial(attention_kernel, layer),
        name=f'attention_{layer}',
        out_shape=jax.ShapeDtypeStruct(q.shape, BF16),
        in_specs=[pl.BlockSpec(memory_space=pltpu.SMEM)] * 2 + [hbm] * 5,
        out_specs=vmem,
        scratch_shapes=[
            pltpu.VMEM(q.shape, BF16),
            pltpu.VMEM(k.shape, BF16),
            pltpu.VMEM(v.shape, BF16),
            pltpu.VMEM((SLOTS, BATCH, kv, seq, head), BF16),
            pltpu.VMEM((SLOTS, BATCH, kv, seq, head), BF16),
            pltpu.VMEM((kv, rows * 8, head), F32),
            pltpu.VMEM((rows, kv * head), F32),
            pltpu.VMEM((rows, kv * head), F32),
            pltpu.VMEM((BATCH * 8, seq), F32),
            pltpu.VMEM((rows * 8, head), F32),
            pltpu.VMEM((kv, seq, head), BF16),
            pltpu.VMEM((kv, seq, head), BF16),
            pltpu.SemaphoreType.DMA((SLOTS, BATCH, 2)),
            pltpu.SemaphoreType.DMA((5,)),
        ],
        compiler_params=pltpu.CompilerParams(vmem_limit_bytes=60 * 2**20),
    )(lengths, order, q, k, v, k_cache, v_cache)


def block_kernel(layer, last, groups, *refs):
    if last:
        (x_hbm, att_hbm, gain_ref, wo_hbm, wg_hbm, wu_hbm, wd_hbm, out_ref,
         xh, att, h, part, got, send, cross, b, act, wo, wg, wu, wd, lsem, osem, msem, csem, fsem) = refs
    else:
        (x_hbm, att_hbm, gain_ref, wo_hbm, wg_hbm, wu_hbm, wd_hbm, next_gain_ref, cos_hbm, sin_hbm, wq_hbm, wk_hbm, wv_hbm, out_ref, q_hbm, k_hbm, v_hbm,
         xh, att, h, part, got, send, cross, b, act, wo, wg, wu, wd, wq, wk, wv, cos_ref, sin_ref, q_ref, k_ref, v_ref, lsem, osem, msem, csem, fsem) = refs
    tp = lax.axis_index('tp')
    core = lax.rem(tp, 2)
    mate = tp + 1 - 2 * core
    peer = lax.rem(tp + 2, 4)
    half = h.shape[2]
    own_cols = pl.ds(pl.multiple_of(core * half, half), half)

    loads = [(x_hbm.at[:, own_cols], xh), (att_hbm, att), (wo_hbm.at[layer], wo), (wg_hbm.at[layer], wg), (wu_hbm.at[layer], wu), (wd_hbm.at[layer], wd)]
    if not last:
        loads += [(wq_hbm.at[layer + 1], wq), (wk_hbm.at[layer + 1], wk), (wv_hbm.at[layer + 1], wv), (cos_hbm, cos_ref), (sin_hbm, sin_ref)]
    loads = [pltpu.make_async_copy(src, dst, lsem.at[n]) for n, (src, dst) in enumerate(loads)]
    for n in (1, 2, 0):
        loads[n].start()

    barrier = pltpu.get_barrier_semaphore()
    for other in (mate, peer):
        pl.semaphore_signal(barrier, inc=1, device_id={'tp': other}, device_id_type=MESH)
    pl.semaphore_wait(barrier, 2)

    def remote(src, dst, sem, idx, device):
        return pltpu.make_async_remote_copy(src_ref=src, dst_ref=dst, send_sem=sem.at[0, idx[0], idx[1]], recv_sem=sem.at[1, idx[0], idx[1]], device_id={'tp': device}, device_id_type=MESH)

    def to_mate(phase, g):
        at = pl.ds(*groups[g])
        return remote(part.at[1 - core, at], got.at[at], msem, (phase, g), mate)

    def to_peer(phase, g):
        at = pl.ds(*groups[g])
        return remote(send.at[at], cross.at[phase, at], csem, (phase, g), peer)

    def final(phase, g):
        at = pl.ds(*groups[g])
        return remote(h.at[core, at], h.at[core, at], fsem, (phase, g), mate)

    def project(lhs_ref, lhs_at, w_ref, g):
        row0, rows = groups[g]
        per_half = half // DOWN_TILE

        def tile(j, _):
            col = pl.multiple_of(j * DOWN_TILE, DOWN_TILE)
            prod = jnp.dot(lhs_ref[lhs_at, :], w_ref[:, pl.ds(col, DOWN_TILE)], preferred_element_type=F32)
            side = j // per_half
            part[side, pl.ds(row0, rows), pl.ds(pl.multiple_of((j - side * per_half) * DOWN_TILE, DOWN_TILE), DOWN_TILE)] = prod.astype(BF16)
            return 0

        lax.fori_loop(0, 2 * per_half, tile, 0, unroll=2)

    def chip_sum(g):
        row0, rows = groups[g]

        def step(i, _):
            at = pl.ds(pl.multiple_of(row0 + i * 16, 16), 16)
            send[at, :] = (part[core, at, :].astype(F32) + got[at, :].astype(F32)).astype(BF16)
            return 0

        lax.fori_loop(0, rows // 16, step, 0, unroll=2)

    def add_sum(phase, g):
        row0, rows = groups[g]

        def step(i, _):
            at = pl.ds(pl.multiple_of(row0 + i * 16, 16), 16)
            base = xh[at, :] if phase == 0 else h[core, at, :]
            total = send[at, :].astype(F32) + cross[phase, at, :].astype(F32)
            h[core, at, :] = (base.astype(F32) + total).astype(BF16)
            return 0

        lax.fori_loop(0, rows // 16, step, 0, unroll=2)

    count = len(groups)

    def arrive(phase, g):
        to_peer(phase, g).wait()
        add_sum(phase, g)
        final(phase, g).start()

    def leave(phase, g):
        to_mate(phase, g).wait()
        chip_sum(g)
        to_peer(phase, g).start()

    loads[1].wait()
    loads[2].wait()
    for n in (3, 4):
        loads[n].start()
    for g in range(count):
        project(att, pl.ds(*groups[g]), wo, g)
        to_mate(0, g).start()
        if g > 0:
            leave(0, g - 1)
    leave(0, count - 1)
    loads[0].wait()
    mlp_gain = gain_ref[...].astype(F32)[layer:layer + 1, :]
    arrive(0, 0)
    loads[5].start()
    for g in range(count):
        row0, rows = groups[g]
        final(0, g).wait()
        norm_rows(h, mlp_gain, b, row0, rows)
        if g == 0:
            loads[3].wait()
            loads[4].wait()

        def up_tile(j, _, rows=rows):
            cols = pl.ds(pl.multiple_of(j * TILE, TILE), TILE)
            gate = jnp.dot(b[0:rows, :], wg[:, cols], preferred_element_type=F32)
            up = jnp.dot(b[0:rows, :], wu[:, cols], preferred_element_type=F32)
            act[0:rows, cols] = (gate * (1.0 / (1.0 + jnp.exp(-gate))) * up).astype(BF16)
            return 0

        lax.fori_loop(0, wg.shape[1] // TILE, up_tile, 0, unroll=2)
        if g == 0:
            loads[5].wait()
            for copy in loads[6:]:
                copy.start()
        project(act, pl.ds(0, rows), wd, g)
        to_mate(1, g).start()
        if g + 1 < count:
            arrive(0, g + 1)
        leave(1, g)
    if not last:
        next_gain = next_gain_ref[...].astype(F32)[layer + 1:layer + 2, :]
        for n in range(6, len(loads)):
            loads[n].wait()
    outs = []
    for g in range(len(groups)):
        row0, rows = groups[g]
        arrive(1, g)
        final(1, g).wait()
        at = pl.ds(row0, rows)
        moves = [(h.at[s, at], out_ref.at[at, pl.ds(s * half, half)]) for s in range(2)]
        if not last:
            norm_rows(h, next_gain, b, row0, rows)
            qkv_rows(b, wq, wk, wv, cos_ref, sin_ref, q_ref, k_ref, v_ref, row0, rows)
            moves += [(src.at[at], dst.at[at]) for src, dst in ((q_ref, q_hbm), (k_ref, k_hbm), (v_ref, v_hbm))]
        for n, (src, dst) in enumerate(moves):
            outs.append(pltpu.make_async_copy(src, dst, osem.at[g, n]))
            outs[-1].start()
    for copy in outs:
        copy.wait()


def block_call(layer, last, x, att, mlp_gain, w_o, w_gate, w_up, w_down, extra):
    rows, width = x.shape
    half = width // 2
    most = max(n for _, n in GROUPS)
    count = len(GROUPS)
    vmem = pl.BlockSpec(memory_space=pltpu.VMEM)
    hbm = pl.BlockSpec(memory_space=pl.ANY)
    out_shape = [jax.ShapeDtypeStruct((rows, width), BF16)]
    in_specs = [hbm, hbm, vmem, hbm, hbm, hbm, hbm]
    out_specs = [hbm]
    tables = []
    weights = [w_o, w_gate, w_up, w_down]
    if not last:
        in_specs += [vmem, hbm, hbm, hbm, hbm, hbm]
        weights += list(extra[3:])
        out_shape += [jax.ShapeDtypeStruct((rows, w.shape[2]), BF16) for w in extra[3:]]
        out_specs += [hbm] * 3
        tables = [pltpu.VMEM(extra[1].shape, F32)] * 2 + [pltpu.VMEM((rows, w.shape[2]), BF16) for w in extra[3:]]
    return pl.pallas_call(
        functools.partial(block_kernel, layer, last, GROUPS),
        name=f'block_{layer}',
        out_shape=out_shape,
        in_specs=in_specs,
        out_specs=out_specs,
        scratch_shapes=[
            pltpu.VMEM((rows, half), BF16),
            pltpu.VMEM(att.shape, BF16),
            pltpu.VMEM((2, rows, half), BF16),
            pltpu.VMEM((2, rows, half), BF16),
            pltpu.VMEM((rows, half), BF16),
            pltpu.VMEM((rows, half), BF16),
            pltpu.VMEM((2, rows, half), BF16),
            pltpu.VMEM((most, width), BF16),
            pltpu.VMEM((most, w_down.shape[1]), BF16),
        ] + [pltpu.VMEM(w.shape[1:], BF16) for w in weights] + tables + [
            pltpu.SemaphoreType.DMA((11,)),
            pltpu.SemaphoreType.DMA((count, 5)),
            pltpu.SemaphoreType.DMA((2, 2, count)),
            pltpu.SemaphoreType.DMA((2, 2, count)),
            pltpu.SemaphoreType.DMA((2, 2, count)),
        ],
        compiler_params=pltpu.CompilerParams(collective_id=layer, has_side_effects=True, vmem_limit_bytes=VMEM_LIMIT),
    )(x, att, mlp_gain, w_o, w_gate, w_up, w_down, *extra)


def solution(mesh):
    col_spec = P(None, None, 'tp')
    row_spec = P(None, 'tp', None)
    cache_spec = P(None, 'dp', 'tp', None, None)
    in_specs = (P('dp', None), P('dp'), P(), col_spec, col_spec, col_spec, row_spec, P(), col_spec, col_spec, row_spec, cache_spec, cache_spec)

    def body(x, lengths, attn_gain, w_q, w_k, w_v, w_o, mlp_gain, w_gate, w_up, w_down, k_cache, v_cache):
        layers = w_q.shape[0]
        q, k, v, cos, sin, order = qkv_call(lengths, x, attn_gain, w_q, w_k, w_v, k_cache.shape[-1])
        for layer in range(layers):
            last = layer == layers - 1
            att = attention_call(layer, lengths, order, q, k, v, k_cache, v_cache)
            extra = () if last else (attn_gain, cos, sin, w_q, w_k, w_v)
            x, *rest = block_call(layer, last, x, att, mlp_gain, w_o, w_gate, w_up, w_down, extra)
            if not last:
                q, k, v = rest
        return x

    return jax.shard_map(body, mesh=mesh, in_specs=in_specs, out_specs=P('dp', None), check_vma=False)
```
